32 devices in a mesh: gx: 8 (over z, x), gy: 4 (over y, core).
Axes of the slice: x: 2, y: 2, z: 4, core: 2. Of those that a mesh axis runs over, the one named last changes fastest.
Arguments:
- field: float32 [128, 64, 128], P('gx', 'gy'), may hold values from -6 to 6
- conductance: float32 [128, 64, 128], P('gx', 'gy'), may hold values from 200 to 5000
- source: float32 [128, 64, 128], P('gx', 'gy'), may hold values from -600 to 600
Outputs:
- advanced: float32 [128, 64, 128], P('gx', 'gy')
The draws below stay inside these ranges and needn't reach their ends.
All inputs are finite; a program needn't handle non-finite values.
Results may differ from the reference program's by a relative error of at most 0.0003.
Values sent between devices are 32-bit elements; how exact they have to be, the bound alone decides.
A program may use at most 64 MiB of HBM per device.

```python
import math
import jax
import jax.numpy as jnp
from jax import lax

NZ = 128
NX = 128
NY = 64


def shard_levels(rng, extent, shards, smallest, top_value):
    gain, own = 1.0, jax.random.fold_in(rng, 6)
    for position, shards_of in shards:
        steps = jnp.exp(jax.random.uniform(jax.random.fold_in(own, position), (shards_of,), jnp.float32, smallest / len(shards), top_value / len(shards)))
        gain = gain * jnp.repeat(steps, extent[position] // shards_of).reshape([-1 if axis == position else 1 for axis in range(len(extent))])
    return gain


def bell_draw(own_key, extent, spread, reach, split=(), dtype=jnp.bfloat16):
    factor_of = shard_levels(own_key, extent, split, -0.22, 0.18) if split else 1.0
    drawn = jax.random.normal(own_key, extent, jnp.float32) * spread * factor_of
    return jnp.minimum(jnp.maximum(drawn, -reach), reach).astype(dtype)


def setup_inputs(seed: int = 0) -> dict:
    key_of = jax.random.split(jax.random.key(seed), 4)
    return {
        "field": bell_draw(key_of[0], (NX, NY, NZ), 1.0, 6.0, ((0, 8), (1, 4)), jnp.float32),
        "conductance": jnp.clip(jnp.exp(math.log(5000.0) - 3.218876 * jax.random.uniform(key_of[1], (NX, NY, NZ), jnp.float32) ** shard_levels(key_of[1], (NX, NY, NZ), ((0, 8), (1, 4)), -0.2, 0.2)), 200.0, 5000.0),
        "source": bell_draw(key_of[2], (NX, NY, NZ), 100.0, 600.0, ((0, 8), (1, 4)), jnp.float32),
    }


def face_coeffs(cond):
    padded = jnp.pad(cond, ((1, 1), (0, 0), (0, 0)))
    return 0.5 * (padded[:-1] + padded[1:])

def apply_front(values, cond):
    faces = face_coeffs(cond)
    padded = jnp.pad(values, ((1, 1), (0, 0), (0, 0)))
    flux = faces * (padded[1:] - padded[:-1])
    return flux[1:] - flux[:-1]

def apply_along(values, cond, axis):
    moved = apply_front(jnp.moveaxis(values, axis, 0), jnp.moveaxis(cond, axis, 0))
    return jnp.moveaxis(moved, 0, axis)

def solve_along(rights, cond, axis):
    faces = face_coeffs(jnp.moveaxis(cond, axis, 0))
    lower = -0.5 * faces[:-1]
    upper = -0.5 * faces[1:]
    diag = 1.0 - lower - upper
    lower = lower.at[0].set(0.0)
    upper = upper.at[-1].set(0.0)
    moved = jnp.moveaxis(jnp.moveaxis(rights, axis, 0), 0, -1)
    solved = lax.linalg.tridiagonal_solve(jnp.moveaxis(lower, 0, -1), jnp.moveaxis(diag, 0, -1), jnp.moveaxis(upper, 0, -1), moved[..., None])[..., 0]
    return jnp.moveaxis(jnp.moveaxis(solved, -1, 0), 0, axis)

def reference(field, conductance, source):
    apply_x = apply_along(field, conductance, 0)
    apply_y = apply_along(field, conductance, 1)
    apply_z = apply_along(field, conductance, 2)
    first = field + 0.5 * apply_x + apply_y + apply_z + source
    section_x = solve_along(first, conductance, 0)
    section_y = solve_along(section_x - 0.5 * apply_y, conductance, 1)
    return solve_along(section_y - 0.5 * apply_z, conductance, 2)
```

```python
import functools

import jax
import jax.numpy as jnp
from jax import lax
from jax.experimental import pallas as pl
from jax.experimental.pallas import tpu as pltpu
from jax.sharding import PartitionSpec as P

MESH = pl.DeviceIdType.MESH


def factor(cells, first, last):
    count = len(cells)
    ones = jnp.ones_like(cells[0])
    excess = jnp.where(first, 1.0 + 0.25 * cells[0], ones)
    mults, inverses = [None], []
    for i in range(count):
        if i == count - 1:
            excess = excess + jnp.where(last, 0.25 * cells[i], 0.0)
            inverses.append(1.0 / excess)
        else:
            face = 0.25 * (cells[i] + cells[i + 1])
            inverse = 1.0 / (excess + face)
            mult = face * inverse
            inverses.append(inverse)
            mults.append(mult)
            excess = 1.0 + mult * excess
    from_last = [None] * count
    from_last[-1] = inverses[-1]
    for i in range(count - 2, -1, -1):
        from_last[i] = mults[i + 1] * from_last[i + 1]
    prods = [ones]
    for i in range(1, count):
        prods.append(mults[i] * prods[-1])
    from_first = [None] * count
    from_first[-1] = prods[-1] * inverses[-1]
    for i in range(count - 2, -1, -1):
        from_first[i] = prods[i] * inverses[i] + mults[i + 1] * from_first[i + 1]
    return mults, inverses, from_first, from_last


def substitute(rights, mults, inverses):
    count = len(rights)
    values = [rights[0]]
    for i in range(1, count):
        values.append(rights[i] + mults[i] * values[-1])
    out = [None] * count
    out[-1] = values[-1] * inverses[-1]
    for i in range(count - 2, -1, -1):
        out[i] = values[i] * inverses[i] + mults[i + 1] * out[i + 1]
    return out


def kernel(nx, ny, lx, ly, depth, f_ref, c_ref, s_ref, o_ref,
           mult_x, inv_x, head_x, tail_x, mult_y, inv_y, head_y, tail_y,
           pcr_lo, pcr_hi, pcr_inv, work, halo_out, halo_in,
           mat_x, mat_y, alpha_x, beta_x, alpha_y, beta_y, own_x, own_y,
           part_x, part_y, out_x, out_y,
           hs_sem, hr_sem, mxs_sem, mxr_sem, mys_sem, myr_sem,
           pxs_sem, pxr_sem, pys_sem, pyr_sem):
    ix = lax.axis_index("gx")
    iy = lax.axis_index("gy")

    def peer_x(k):
        return (lax.rem(ix + k, nx), iy)

    def peer_y(k):
        return (ix, lax.rem(iy + k, ny))

    barrier = pltpu.get_barrier_semaphore()
    for k in range(1, nx):
        pl.semaphore_signal(barrier, inc=1, device_id=peer_x(k), device_id_type=MESH)
    for k in range(1, ny):
        pl.semaphore_signal(barrier, inc=1, device_id=peer_y(k), device_id_type=MESH)

    def row_x(i):
        return pl.ds(i * ly, ly)

    def row_y(j):
        return pl.ds(j, lx, stride=ly)

    def keep(refs, lists):
        for ref, items in zip(refs, lists):
            for i, item in enumerate(items):
                if item is not None:
                    ref[i] = item

    def describe(mat, index, cells, heads, tails):
        mat[index, 0] = heads[0]
        mat[index, 1] = tails[0]
        mat[index, 2] = tails[-1]
        mat[index, 3] = cells[0]
        mat[index, 4] = cells[-1]

    def spread(src_of, table, index, peer, count, s_sem, r_sem):
        copies = []
        for k in range(1, count):
            copy = pltpu.make_async_remote_copy(
                src_ref=src_of(k), dst_ref=table.at[index],
                send_sem=s_sem.at[k - 1], recv_sem=r_sem.at[k - 1],
                device_id=peer(k), device_id_type=MESH)
            copy.start()
            copies.append(copy)
        return copies

    cells = [c_ref[row_x(i)] for i in range(lx)]
    parts = factor(cells, ix == 0, ix == nx - 1)
    keep((mult_x, inv_x, head_x, tail_x), parts)
    describe(mat_x, ix, cells, parts[2], parts[3])
    for side, j in ((0, 0), (1, ly - 1)):
        halo_out[side, 0] = f_ref[row_y(j)]
        halo_out[side, 1] = c_ref[row_y(j)]

    pl.semaphore_wait(barrier, nx + ny - 2)

    halos = []
    for side, k in ((0, ny - 1), (1, 1)):
        copy = pltpu.make_async_remote_copy(
            src_ref=halo_out.at[side], dst_ref=halo_in.at[side],
            send_sem=hs_sem.at[side], recv_sem=hr_sem.at[side],
            device_id=peer_y(k), device_id_type=MESH)
        copy.start()
        halos.append(copy)
    mats_x = spread(lambda k: mat_x.at[ix], mat_x, ix, peer_x, nx, mxs_sem, mxr_sem)

    cells_y = [c_ref[row_y(j)] for j in range(ly)]
    parts = factor(cells_y, iy == 0, iy == ny - 1)
    keep((mult_y, inv_y, head_y, tail_y), parts)
    describe(mat_y, iy, cells_y, parts[2], parts[3])
    mats_y = spread(lambda k: mat_y.at[iy], mat_y, iy, peer_y, ny, mys_sem, myr_sem)

    lane = lax.broadcasted_iota(jnp.int32, (ly, depth), 1)
    low_end = lane == 0
    high_end = lane == depth - 1
    for i in range(lx):
        cond = c_ref[row_x(i)]
        value = f_ref[row_x(i)]
        lo = jnp.where(low_end, 0.0, 0.25 * (cond + pltpu.roll(cond, 1, 1)))
        hi = jnp.where(high_end, 0.0, 0.25 * (cond + pltpu.roll(cond, depth - 1, 1)))
        edge = jnp.where(low_end, 0.25 * cond, 0.0) + jnp.where(high_end, 0.25 * cond, 0.0)
        flux = (hi * (pltpu.roll(value, depth - 1, 1) - value)
                - lo * (value - pltpu.roll(value, 1, 1)) - edge * value)
        work[row_x(i)] = 2.0 * (value + flux) + s_ref[row_x(i)]
        excess = 1.0 + edge
        shift, level = 1, 0
        while shift < depth:
            inverse = 1.0 / (excess + lo + hi)
            a = lo * pltpu.roll(inverse, shift, 1)
            b = hi * pltpu.roll(inverse, depth - shift, 1)
            pcr_lo[level, row_x(i)] = a
            pcr_hi[level, row_x(i)] = b
            excess = (excess + a * pltpu.roll(excess, shift, 1)
                      + b * pltpu.roll(excess, depth - shift, 1))
            lo = a * pltpu.roll(lo, shift, 1)
            hi = b * pltpu.roll(hi, depth - shift, 1)
            shift, level = 2 * shift, level + 1
        pcr_inv[row_x(i)] = 1.0 / (excess + lo + hi)

    for copy in halos:
        copy.wait()
    below_f = jnp.where(iy == 0, 0.0, halo_in[1, 0])
    below_c = jnp.where(iy == 0, 0.0, halo_in[1, 1])
    above_f = jnp.where(iy == ny - 1, 0.0, halo_in[0, 0])
    above_c = jnp.where(iy == ny - 1, 0.0, halo_in[0, 1])
    value = f_ref[row_y(0)]
    cond = c_ref[row_y(0)]
    flux_lo = 0.5 * (below_c + cond) * (value - below_f)
    for j in range(ly):
        if j == ly - 1:
            next_f, next_c = above_f, above_c
        else:
            next_f, next_c = f_ref[row_y(j + 1)], c_ref[row_y(j + 1)]
        flux_hi = 0.5 * (cond + next_c) * (next_f - value)
        work[row_y(j)] += flux_hi - flux_lo
        value, cond, flux_lo = next_f, next_c, flux_hi

    def chains(mat, count, alpha, beta, own, index):
        links = [4.0 / (mat[k, 4] + mat[k + 1, 3]) for k in range(count - 1)]
        zeros = jnp.zeros_like(links[0])
        alpha[0] = zeros
        own[0, 0] = zeros
        joined = mat[0, 2]
        for k in range(1, count):
            inverse = 1.0 / (links[k - 1] + joined + mat[k, 0])
            ratio = mat[k, 1] * inverse
            alpha[k] = ratio
            own[0, k] = inverse
            joined = mat[k, 2] - mat[k, 1] * ratio
        beta[count - 1] = zeros
        own[1, count - 1] = zeros
        joined = mat[count - 1, 0]
        for k in range(count - 2, -1, -1):
            inverse = 1.0 / (links[k] + joined + mat[k, 2])
            ratio = mat[k, 1] * inverse
            beta[k] = ratio
            own[1, k] = inverse
            joined = mat[k, 0] - mat[k, 1] * ratio

    def send_parts(head, tail, alpha, beta, index, count, outs, table, peer, s_sem, r_sem):
        outs[0] = tail - alpha[index] * head
        outs[1] = head - beta[index] * tail
        table[index] = head

        def src_of(k):
            return outs.at[lax.div(index + k, count)]
        return spread(src_of, table, index, peer, count, s_sem, r_sem)

    def fluxes(head, tail, alpha, beta, own, index, count, table):
        before = jnp.zeros_like(head)
        for k in range(count - 1):
            before = jnp.where(k < index, alpha[k] * before + table[k], before)
        after = jnp.zeros_like(head)
        for k in range(count - 1, 0, -1):
            after = jnp.where(k > index, beta[k] * after + table[k], after)
        a, b = alpha[index], beta[index]
        scale = 1.0 / (1.0 - a * b)
        left = before - head
        right = tail - after
        into = scale * own[0, index] * (left + b * right)
        out = scale * own[1, index] * (right + a * left)
        return into, out

    local = substitute([work[row_x(i)] for i in range(lx)],
                       [None] + [mult_x[i] for i in range(1, lx)],
                       [inv_x[i] for i in range(lx)])
    for copy in mats_x:
        copy.wait()
    chains(mat_x, nx, alpha_x, beta_x, own_x, ix)
    copies = send_parts(local[0], local[-1], alpha_x, beta_x, ix, nx,
                        out_x, part_x, peer_x, pxs_sem, pxr_sem)
    for i in range(lx):
        work[row_x(i)] = local[i] - 2.0 * f_ref[row_x(i)]
    head, tail = local[0], local[-1]
    for copy in mats_y:
        copy.wait()
    chains(mat_y, ny, alpha_y, beta_y, own_y, iy)
    for copy in copies:
        copy.wait()
    into, out = fluxes(head, tail, alpha_x, beta_x, own_x, ix, nx, part_x)
    for i in range(lx):
        work[row_x(i)] += into * head_x[i] - out * tail_x[i]

    local = substitute([work[row_y(j)] for j in range(ly)],
                       [None] + [mult_y[j] for j in range(1, ly)],
                       [inv_y[j] for j in range(ly)])
    copies = send_parts(local[0], local[-1], alpha_y, beta_y, iy, ny,
                        out_y, part_y, peer_y, pys_sem, pyr_sem)
    for j in range(ly):
        work[row_y(j)] = local[j]
    head, tail = local[0], local[-1]
    for copy in copies:
        copy.wait()
    into, out = fluxes(head, tail, alpha_y, beta_y, own_y, iy, ny, part_y)
    for j in range(ly):
        work[row_y(j)] += into * head_y[j] - out * tail_y[j]

    shift, level = 1, 0
    right = work[...]
    while shift < depth:
        right = (right + pcr_lo[level] * pltpu.roll(right, shift, 1)
                 + pcr_hi[level] * pltpu.roll(right, depth - shift, 1))
        shift, level = 2 * shift, level + 1
    o_ref[...] = f_ref[...] + right * pcr_inv[...]


def solution(mesh):
    nx, ny = mesh.shape["gx"], mesh.shape["gy"]

    def body(field, conductance, source):
        lx, ly, depth = field.shape
        lines = lx * ly
        levels = max(1, (depth - 1).bit_length())
        f32 = jnp.float32

        def vmem(*shape):
            return pltpu.VMEM(shape, f32)

        def dma(count):
            return pltpu.SemaphoreType.DMA((count,))

        along_x = [vmem(lx, ly, depth)] * 4
        along_y = [vmem(ly, lx, depth)] * 4
        out = pl.pallas_call(
            functools.partial(kernel, nx, ny, lx, ly, depth),
            out_shape=jax.ShapeDtypeStruct((lines, depth), f32),
            in_specs=[pl.BlockSpec(memory_space=pltpu.VMEM)] * 3,
            out_specs=pl.BlockSpec(memory_space=pltpu.VMEM),
            scratch_shapes=along_x + along_y + [
                vmem(levels, lines, depth), vmem(levels, lines, depth), vmem(lines, depth),
                vmem(lines, depth), vmem(2, 2, lx, depth), vmem(2, 2, lx, depth),
                vmem(nx, 5, ly, depth), vmem(ny, 5, lx, depth),
                vmem(nx, ly, depth), vmem(nx, ly, depth),
                vmem(ny, lx, depth), vmem(ny, lx, depth),
                vmem(2, nx, ly, depth), vmem(2, ny, lx, depth),
                vmem(nx, ly, depth), vmem(ny, lx, depth),
                vmem(2, ly, depth), vmem(2, lx, depth),
                dma(2), dma(2), dma(nx - 1), dma(nx - 1), dma(ny - 1), dma(ny - 1),
                dma(nx - 1), dma(nx - 1), dma(ny - 1), dma(ny - 1),
            ],
            compiler_params=pltpu.CompilerParams(collective_id=0, has_side_effects=True),
            name="step",
        )(field.reshape(lines, depth), conductance.reshape(lines, depth),
          source.reshape(lines, depth))
        return out.reshape(lx, ly, depth)

    spec = P("gx", "gy", None)
    return jax.shard_map(body, mesh=mesh, in_specs=(spec, spec, spec), out_specs=spec,
                         check_vma=False)
```

```python
import functools

import jax
import jax.numpy as jnp
from jax import lax
from jax.experimental import pallas as pl
from jax.experimental.pallas import tpu as pltpu
from jax.sharding import PartitionSpec as P

MESH = pl.DeviceIdType.MESH


def factor(cells, first, last):
    count = len(cells)
    ones = jnp.ones_like(cells[0])
    excess = jnp.where(first, 1.0 + 0.25 * cells[0], ones)
    mults, inverses = [None], []
    for i in range(count):
        if i == count - 1:
            excess = excess + jnp.where(last, 0.25 * cells[i], 0.0)
            inverses.append(1.0 / excess)
        else:
            face = 0.25 * (cells[i] + cells[i + 1])
            inverse = 1.0 / (excess + face)
            mult = face * inverse
            inverses.append(inverse)
            mults.append(mult)
            excess = 1.0 + mult * excess
    from_last = [None] * count
    from_last[-1] = inverses[-1]
    for i in range(count - 2, -1, -1):
        from_last[i] = mults[i + 1] * from_last[i + 1]
    prods = [ones]
    for i in range(1, count):
        prods.append(mults[i] * prods[-1])
    from_first = [None] * count
    from_first[-1] = prods[-1] * inverses[-1]
    for i in range(count - 2, -1, -1):
        from_first[i] = prods[i] * inverses[i] + mults[i + 1] * from_first[i + 1]
    return mults, inverses, from_first, from_last


def substitute(rights, mults, inverses):
    count = len(rights)
    values = [rights[0]]
    for i in range(1, count):
        values.append(rights[i] + mults[i] * values[-1])
    out = [None] * count
    out[-1] = values[-1] * inverses[-1]
    for i in range(count - 2, -1, -1):
        out[i] = values[i] * inverses[i] + mults[i + 1] * out[i + 1]
    return out


def kernel(nx, ny, lx, ly, depth, f_hbm, c_hbm, s_hbm, o_ref,
           f_ref, c_ref, s_ref,
           mult_x, inv_x, head_x, tail_x, mult_y, inv_y, head_y, tail_y,
           pcr_lo, pcr_hi, pcr_inv, work, halo_out, halo_in,
           mat_x, mat_y, outer_x, inner_x, alpha_y, beta_y, own_y,
           part_x, part_y, out_y, mid_out, mid_in, chain_out, chain_in,
           in_sem, hs_sem, hr_sem, mxs_sem, mxr_sem, mys_sem, myr_sem,
           pxs_sem, pxr_sem, pys_sem, pyr_sem, mid_sem):
    ix = lax.axis_index("gx")
    iy = lax.axis_index("gy")
    half = nx // 2
    upper = lax.div(ix, half)
    place = ix - upper * half
    rank = ix + upper * (nx - 1 - 2 * ix)
    flip = upper == 1

    def peer_x(k):
        return (upper * half + lax.rem(place + k, half), iy)

    mirror = (lax.rem(ix + half, nx), iy)

    def peer_y(k):
        return (ix, lax.rem(iy + k, ny))

    barrier = pltpu.get_barrier_semaphore()
    pl.semaphore_signal(barrier, inc=1, device_id=mirror, device_id_type=MESH)
    for k in range(1, half):
        pl.semaphore_signal(barrier, inc=1, device_id=peer_x(k), device_id_type=MESH)
    for k in range(1, ny):
        pl.semaphore_signal(barrier, inc=1, device_id=peer_y(k), device_id_type=MESH)

    fetches = []
    for n, (src, dst) in enumerate(((c_hbm, c_ref), (f_hbm, f_ref), (s_hbm, s_ref))):
        fetch = pltpu.make_async_copy(src, dst, in_sem.at[n])
        fetch.start()
        fetches.append(fetch)

    def row_x(i):
        return pl.ds(i * ly, ly)

    def row_y(j):
        return pl.ds(j, lx, stride=ly)

    def keep(refs, lists):
        for ref, items in zip(refs, lists):
            for i, item in enumerate(items):
                if item is not None:
                    ref[i] = item

    def remote(src, dst, s_sem, r_sem, device):
        copy = pltpu.make_async_remote_copy(
            src_ref=src, dst_ref=dst, send_sem=s_sem, recv_sem=r_sem,
            device_id=device, device_id_type=MESH)
        copy.start()
        return copy

    def spread(src_of, table, index, peer, count, s_sem, r_sem):
        return [remote(src_of(k), table.at[index], s_sem.at[k - 1], r_sem.at[k - 1], peer(k))
                for k in range(1, count)]

    def turn(first, second):
        return jnp.where(flip, second, first), jnp.where(flip, first, second)

    fetches[0].wait()
    cells = [c_ref[row_x(i)] for i in range(lx)]
    parts = factor(cells, ix == 0, ix == nx - 1)
    keep((mult_x, inv_x, head_x, tail_x), parts)
    heads, tails = parts[2], parts[3]
    mat_x[rank, 0], mat_x[rank, 2] = turn(heads[0], tails[-1])
    mat_x[rank, 1] = tails[0]
    mat_x[rank, 3], mat_x[rank, 4] = turn(cells[0], cells[-1])
    fetches[1].wait()
    for side, j in ((0, 0), (1, ly - 1)):
        halo_out[side, 0] = f_ref[row_y(j)]
        halo_out[side, 1] = c_ref[row_y(j)]

    pl.semaphore_wait(barrier, half + ny - 1)

    halos = [remote(halo_out.at[side], halo_in.at[side], hs_sem.at[side], hr_sem.at[side],
                    peer_y(k)) for side, k in ((0, ny - 1), (1, 1))]
    mats_x = spread(lambda k: mat_x.at[rank], mat_x, rank, peer_x, half, mxs_sem, mxr_sem)

    cells = [c_ref[row_y(j)] for j in range(ly)]
    parts = factor(cells, iy == 0, iy == ny - 1)
    keep((mult_y, inv_y, head_y, tail_y), parts)
    heads, tails = parts[2], parts[3]
    mat_y[iy, 0] = heads[0]
    mat_y[iy, 1] = tails[0]
    mat_y[iy, 2] = tails[-1]
    mat_y[iy, 3] = cells[0]
    mat_y[iy, 4] = cells[-1]
    mats_y = spread(lambda k: mat_y.at[iy], mat_y, iy, peer_y, ny, mys_sem, myr_sem)

    lane = lax.broadcasted_iota(jnp.int32, (ly, depth), 1)
    low_end = lane == 0
    high_end = lane == depth - 1

    def faces_z(cond):
        lo = jnp.where(low_end, 0.0, 0.25 * (cond + pltpu.roll(cond, 1, 1)))
        hi = jnp.where(high_end, 0.0, 0.25 * (cond + pltpu.roll(cond, depth - 1, 1)))
        edge = jnp.where(low_end, 0.25 * cond, 0.0) + jnp.where(high_end, 0.25 * cond, 0.0)
        return lo, hi, edge

    fetches[2].wait()
    for i in range(lx):
        value = f_ref[row_x(i)]
        lo, hi, edge = faces_z(c_ref[row_x(i)])
        flux = (hi * (pltpu.roll(value, depth - 1, 1) - value)
                - lo * (value - pltpu.roll(value, 1, 1)) - edge * value)
        work[row_x(i)] = 2.0 * (value + flux) + s_ref[row_x(i)]

    for copy in halos:
        copy.wait()
    below_f = jnp.where(iy == 0, 0.0, halo_in[1, 0])
    below_c = jnp.where(iy == 0, 0.0, halo_in[1, 1])
    above_f = jnp.where(iy == ny - 1, 0.0, halo_in[0, 0])
    above_c = jnp.where(iy == ny - 1, 0.0, halo_in[0, 1])
    value = f_ref[row_y(0)]
    cond = c_ref[row_y(0)]
    flux_lo = 0.5 * (below_c + cond) * (value - below_f)
    for j in range(ly):
        if j == ly - 1:
            next_f, next_c = above_f, above_c
        else:
            next_f, next_c = f_ref[row_y(j + 1)], c_ref[row_y(j + 1)]
        flux_hi = 0.5 * (cond + next_c) * (next_f - value)
        work[row_y(j)] += flux_hi - flux_lo
        value, cond, flux_lo = next_f, next_c, flux_hi

    local = substitute([work[row_x(i)] for i in range(lx)],
                       [None] + [mult_x[i] for i in range(1, lx)],
                       [inv_x[i] for i in range(lx)])
    near, far = turn(local[0], local[-1])
    part_x[rank, 0] = near
    part_x[rank, 1] = far
    parts_x = spread(lambda k: part_x.at[rank], part_x, rank, peer_x, half, pxs_sem, pxr_sem)
    for i in range(lx):
        work[row_x(i)] = local[i] - 2.0 * f_ref[row_x(i)]

    for i in range(lx):
        lo, hi, edge = faces_z(c_ref[row_x(i)])
        excess = 1.0 + edge
        shift, level = 1, 0
        while shift < depth:
            inverse = 1.0 / (excess + lo + hi)
            a = lo * pltpu.roll(inverse, shift, 1)
            b = hi * pltpu.roll(inverse, depth - shift, 1)
            pcr_lo[level, row_x(i)] = a
            pcr_hi[level, row_x(i)] = b
            excess = (excess + a * pltpu.roll(excess, shift, 1)
                      + b * pltpu.roll(excess, depth - shift, 1))
            lo = a * pltpu.roll(lo, shift, 1)
            hi = b * pltpu.roll(hi, depth - shift, 1)
            shift, level = 2 * shift, level + 1
        pcr_inv[row_x(i)] = 1.0 / (excess + lo + hi)

    for copy in mats_x:
        copy.wait()
    zeros = jnp.zeros_like(near)
    outer_x[0, 0] = zeros
    outer_x[1, 0] = zeros
    outer_x[2, 0] = zeros
    ratios = [zeros]
    joined = mat_x[0, 2]
    for q in range(1, half):
        link = 4.0 / (mat_x[q - 1, 4] + mat_x[q, 3])
        inverse = 1.0 / (link + joined + mat_x[q, 0])
        ratio = mat_x[q, 1] * inverse
        outer_x[0, q] = inverse
        outer_x[1, q] = ratio
        ratios.append(ratio)
        joined = mat_x[q, 2] - mat_x[q, 1] * ratio
    mid_out[0] = joined
    mid_out[1] = mat_x[half - 1, 4]
    mids = remote(mid_out, mid_in, mid_sem.at[0], mid_sem.at[1], mirror)

    for copy in mats_y:
        copy.wait()
    links = [4.0 / (mat_y[k, 4] + mat_y[k + 1, 3]) for k in range(ny - 1)]
    blank = jnp.zeros_like(links[0])
    alpha_y[0] = blank
    own_y[0, 0] = blank
    joined = mat_y[0, 2]
    for k in range(1, ny):
        inverse = 1.0 / (links[k - 1] + joined + mat_y[k, 0])
        ratio = mat_y[k, 1] * inverse
        alpha_y[k] = ratio
        own_y[0, k] = inverse
        joined = mat_y[k, 2] - mat_y[k, 1] * ratio
    beta_y[ny - 1] = blank
    own_y[1, ny - 1] = blank
    joined = mat_y[ny - 1, 0]
    for k in range(ny - 2, -1, -1):
        inverse = 1.0 / (links[k] + joined + mat_y[k, 2])
        ratio = mat_y[k, 1] * inverse
        beta_y[k] = ratio
        own_y[1, k] = inverse
        joined = mat_y[k, 0] - mat_y[k, 1] * ratio

    for copy in parts_x:
        copy.wait()
    before = part_x[0, 1]
    for q in range(1, half):
        outer_x[2, q] = before
        before = part_x[q, 1] + ratios[q] * (before - part_x[q, 0])
    chain_out[...] = before
    chained = remote(chain_out, chain_in, mid_sem.at[2], mid_sem.at[3], mirror)

    mids.wait()
    joined = mid_in[0]
    beyond = mid_in[1]
    ratios = [None] * half
    for q in range(half - 1, -1, -1):
        inverse = 1.0 / (4.0 / (mat_x[q, 4] + beyond) + joined + mat_x[q, 2])
        ratio = mat_x[q, 1] * inverse
        inner_x[0, q] = inverse
        inner_x[1, q] = ratio
        ratios[q] = ratio
        joined = mat_x[q, 0] - mat_x[q, 1] * ratio
        beyond = mat_x[q, 3]
    a, b = outer_x[1, rank], inner_x[1, rank]
    scale = 1.0 / (1.0 - a * b)
    gain_near = scale * outer_x[0, rank]
    gain_far = scale * inner_x[0, rank]
    left = outer_x[2, rank] - near
    chained.wait()
    after = chain_in[...]
    for q in range(half - 1, -1, -1):
        inner_x[2, q] = after
        if q:
            after = part_x[q, 0] + ratios[q] * (after - part_x[q, 1])
    right = far - inner_x[2, rank]
    into = gain_near * (left + b * right)
    out = gain_far * (right + a * left)
    on_head, on_tail = turn(into, -out)
    for i in range(lx):
        work[row_x(i)] += on_head * head_x[i] + on_tail * tail_x[i]

    local = substitute([work[row_y(j)] for j in range(ly)],
                       [None] + [mult_y[j] for j in range(1, ly)],
                       [inv_y[j] for j in range(ly)])
    head, tail = local[0], local[-1]
    a, b = alpha_y[iy], beta_y[iy]
    out_y[0] = tail - a * head
    out_y[1] = head - b * tail
    part_y[iy] = head
    copies = spread(lambda k: out_y.at[lax.div(iy + k, ny)], part_y, iy, peer_y, ny,
                    pys_sem, pyr_sem)
    for j in range(ly):
        work[row_y(j)] = local[j]
    scale = 1.0 / (1.0 - a * b)
    gain_in, gain_out = scale * own_y[0, iy], scale * own_y[1, iy]
    for copy in copies:
        copy.wait()
    before = blank
    for k in range(ny - 1):
        before = jnp.where(k < iy, alpha_y[k] * before + part_y[k], before)
    after = blank
    for k in range(ny - 1, 0, -1):
        after = jnp.where(k > iy, beta_y[k] * after + part_y[k], after)
    left = before - head
    right = tail - after
    into = gain_in * (left + b * right)
    out = gain_out * (right + a * left)
    for j in range(ly):
        work[row_y(j)] += into * head_y[j] - out * tail_y[j]

    shift, level = 1, 0
    right = work[...]
    while shift < depth:
        right = (right + pcr_lo[level] * pltpu.roll(right, shift, 1)
                 + pcr_hi[level] * pltpu.roll(right, depth - shift, 1))
        shift, level = 2 * shift, level + 1
    o_ref[...] = f_ref[...] + right * pcr_inv[...]


def solution(mesh):
    nx, ny = mesh.shape["gx"], mesh.shape["gy"]

    def body(field, conductance, source):
        lx, ly, depth = field.shape
        lines = lx * ly
        levels = max(1, (depth - 1).bit_length())
        f32 = jnp.float32

        def vmem(*shape):
            return pltpu.VMEM(shape, f32)

        def dma(count):
            return pltpu.SemaphoreType.DMA((count,))

        half = nx // 2
        along_x = [vmem(lx, ly, depth)] * 4
        along_y = [vmem(ly, lx, depth)] * 4
        out = pl.pallas_call(
            functools.partial(kernel, nx, ny, lx, ly, depth),
            out_shape=jax.ShapeDtypeStruct((lines, depth), f32),
            in_specs=[pl.BlockSpec(memory_space=pltpu.HBM)] * 3,
            out_specs=pl.BlockSpec(memory_space=pltpu.VMEM),
            scratch_shapes=[vmem(lines, depth)] * 3 + along_x + along_y + [
                vmem(levels, lines, depth), vmem(levels, lines, depth), vmem(lines, depth),
                vmem(lines, depth), vmem(2, 2, lx, depth), vmem(2, 2, lx, depth),
                vmem(half, 5, ly, depth), vmem(ny, 5, lx, depth),
                vmem(3, half, ly, depth), vmem(3, half, ly, depth),
                vmem(ny, lx, depth), vmem(ny, lx, depth), vmem(2, ny, lx, depth),
                vmem(half, 2, ly, depth), vmem(ny, lx, depth), vmem(2, lx, depth),
                vmem(2, ly, depth), vmem(2, ly, depth), vmem(ly, depth), vmem(ly, depth),
                dma(3), dma(2), dma(2), dma(half - 1), dma(half - 1), dma(ny - 1), dma(ny - 1),
                dma(half - 1), dma(half - 1), dma(ny - 1), dma(ny - 1), dma(4),
            ],
            compiler_params=pltpu.CompilerParams(
                collective_id=0, has_side_effects=True),
            name="step",
        )(field.reshape(lines, depth), conductance.reshape(lines, depth),
          source.reshape(lines, depth))
        return out.reshape(lx, ly, depth)

    spec = P("gx", "gy", None)
    return jax.shard_map(body, mesh=mesh, in_specs=(spec, spec, spec), out_specs=spec,
                         check_vma=False)
```

```python
import functools

import jax
import jax.numpy as jnp
from jax import lax
from jax.experimental import pallas as pl
from jax.experimental.pallas import tpu as pltpu
from jax.sharding import PartitionSpec as P

MESH = pl.DeviceIdType.MESH


def factor(cells, first, last):
    count = len(cells)
    ones = jnp.ones_like(cells[0])
    excess = jnp.where(first, 1.0 + 0.25 * cells[0], ones)
    mults, inverses = [None], []
    for i in range(count):
        if i == count - 1:
            excess = excess + jnp.where(last, 0.25 * cells[i], 0.0)
            inverses.append(1.0 / excess)
        else:
            face = 0.25 * (cells[i] + cells[i + 1])
            inverse = 1.0 / (excess + face)
            mult = face * inverse
            inverses.append(inverse)
            mults.append(mult)
            excess = 1.0 + mult * excess
    from_last = [None] * count
    from_last[-1] = inverses[-1]
    for i in range(count - 2, -1, -1):
        from_last[i] = mults[i + 1] * from_last[i + 1]
    prods = [ones]
    for i in range(1, count):
        prods.append(mults[i] * prods[-1])
    from_first = [None] * count
    from_first[-1] = prods[-1] * inverses[-1]
    for i in range(count - 2, -1, -1):
        from_first[i] = prods[i] * inverses[i] + mults[i + 1] * from_first[i + 1]
    return mults, inverses, from_first, from_last


def substitute(rights, mults, inverses):
    count = len(rights)
    values = [rights[0]]
    for i in range(1, count):
        values.append(rights[i] + mults[i] * values[-1])
    out = [None] * count
    out[-1] = values[-1] * inverses[-1]
    for i in range(count - 2, -1, -1):
        out[i] = values[i] * inverses[i] + mults[i + 1] * out[i + 1]
    return out


def kernel(nx, ny, lx, ly, depth, f_hbm, c_hbm, s_hbm, o_ref,
           f_ref, c_ref, s_ref,
           mult_x, inv_x, head_x, tail_x, mult_y, inv_y, head_y, tail_y,
           pcr_lo, pcr_hi, pcr_inv, work, halo_out, halo_in,
           mat_x, mat_y, outer_x, inner_x, alpha_y, beta_y, own_y,
           part_x, part_y, out_y, mid_out, mid_in, chain_out, chain_in,
           in_sem, hs_sem, hr_sem, mxs_sem, mxr_sem, mys_sem, myr_sem,
           pxs_sem, pxr_sem, pys_sem, pyr_sem, mid_sem):
    ix = lax.axis_index("gx")
    iy = lax.axis_index("gy")
    half = nx // 2
    upper = lax.div(ix, half)
    place = ix - upper * half
    rank = ix + upper * (nx - 1 - 2 * ix)
    flip = upper == 1

    def peer_x(k):
        return (upper * half + lax.rem(place + k, half), iy)

    mirror = (lax.rem(ix + half, nx), iy)

    def peer_y(k):
        return (ix, lax.rem(iy + k, ny))

    barrier = pltpu.get_barrier_semaphore()
    pl.semaphore_signal(barrier, inc=1, device_id=mirror, device_id_type=MESH)
    for k in range(1, half):
        pl.semaphore_signal(barrier, inc=1, device_id=peer_x(k), device_id_type=MESH)
    for k in range(1, ny):
        pl.semaphore_signal(barrier, inc=1, device_id=peer_y(k), device_id_type=MESH)

    fetches = []
    for n, (src, dst) in enumerate(((c_hbm, c_ref), (f_hbm, f_ref), (s_hbm, s_ref))):
        fetch = pltpu.make_async_copy(src, dst, in_sem.at[n])
        fetch.start()
        fetches.append(fetch)

    def row_x(i):
        return pl.ds(i * ly, ly)

    def row_y(j):
        return pl.ds(j, lx, stride=ly)

    def keep(refs, lists):
        for ref, items in zip(refs, lists):
            for i, item in enumerate(items):
                if item is not None:
                    ref[i] = item

    def remote(src, dst, s_sem, r_sem, device):
        copy = pltpu.make_async_remote_copy(
            src_ref=src, dst_ref=dst, send_sem=s_sem, recv_sem=r_sem,
            device_id=device, device_id_type=MESH)
        copy.start()
        return copy

    def spread(src_of, table, index, peer, count, s_sem, r_sem):
        return [remote(src_of(k), table.at[index], s_sem.at[k - 1], r_sem.at[k - 1], peer(k))
                for k in range(1, count)]

    def turn(first, second):
        return jnp.where(flip, second, first), jnp.where(flip, first, second)

    fetches[0].wait()
    cells = [c_ref[row_x(i)] for i in range(lx)]
    parts = factor(cells, ix == 0, ix == nx - 1)
    keep((mult_x, inv_x, head_x, tail_x), parts)
    heads, tails = parts[2], parts[3]
    mat_x[rank, 0], mat_x[rank, 2] = turn(heads[0], tails[-1])
    mat_x[rank, 1] = tails[0]
    mat_x[rank, 3], mat_x[rank, 4] = turn(cells[0], cells[-1])
    fetches[1].wait()
    for side, j in ((0, 0), (1, ly - 1)):
        halo_out[side, 0] = f_ref[row_y(j)]
        halo_out[side, 1] = c_ref[row_y(j)]

    pl.semaphore_wait(barrier, half + ny - 1)

    halos = [remote(halo_out.at[side], halo_in.at[side], hs_sem.at[side], hr_sem.at[side],
                    peer_y(k)) for side, k in ((0, ny - 1), (1, 1))]
    mats_x = spread(lambda k: mat_x.at[rank], mat_x, rank, peer_x, half, mxs_sem, mxr_sem)

    cells = [c_ref[row_y(j)] for j in range(ly)]
    parts = factor(cells, iy == 0, iy == ny - 1)
    keep((mult_y, inv_y, head_y, tail_y), parts)
    heads, tails = parts[2], parts[3]
    mat_y[iy, 0] = heads[0]
    mat_y[iy, 1] = tails[0]
    mat_y[iy, 2] = tails[-1]
    mat_y[iy, 3] = cells[0]
    mat_y[iy, 4] = cells[-1]
    mats_y = spread(lambda k: mat_y.at[iy], mat_y, iy, peer_y, ny, mys_sem, myr_sem)

    lane = lax.broadcasted_iota(jnp.int32, (ly, depth), 1)
    low_end = lane == 0
    high_end = lane == depth - 1

    def faces_z(cond):
        lo = jnp.where(low_end, 0.0, 0.25 * (cond + pltpu.roll(cond, 1, 1)))
        hi = jnp.where(high_end, 0.0, 0.25 * (cond + pltpu.roll(cond, depth - 1, 1)))
        edge = jnp.where(low_end, 0.25 * cond, 0.0) + jnp.where(high_end, 0.25 * cond, 0.0)
        return lo, hi, edge

    fetches[2].wait()
    for i in range(lx):
        value = f_ref[row_x(i)]
        lo, hi, edge = faces_z(c_ref[row_x(i)])
        flux = (hi * (pltpu.roll(value, depth - 1, 1) - value)
                - lo * (value - pltpu.roll(value, 1, 1)) - edge * value)
        work[row_x(i)] = 2.0 * (value + flux) + s_ref[row_x(i)]

    for copy in halos:
        copy.wait()
    below_f = jnp.where(iy == 0, 0.0, halo_in[1, 0])
    below_c = jnp.where(iy == 0, 0.0, halo_in[1, 1])
    above_f = jnp.where(iy == ny - 1, 0.0, halo_in[0, 0])
    above_c = jnp.where(iy == ny - 1, 0.0, halo_in[0, 1])
    value = f_ref[row_y(0)]
    cond = c_ref[row_y(0)]
    flux_lo = 0.5 * (below_c + cond) * (value - below_f)
    for j in range(ly):
        if j == ly - 1:
            next_f, next_c = above_f, above_c
        else:
            next_f, next_c = f_ref[row_y(j + 1)], c_ref[row_y(j + 1)]
        flux_hi = 0.5 * (cond + next_c) * (next_f - value)
        work[row_y(j)] += flux_hi - flux_lo
        value, cond, flux_lo = next_f, next_c, flux_hi

    local = substitute([work[row_x(i)] for i in range(lx)],
                       [None] + [mult_x[i] for i in range(1, lx)],
                       [inv_x[i] for i in range(lx)])
    near, far = turn(local[0], local[-1])
    part_x[rank, 0] = near
    part_x[rank, 1] = far
    parts_x = spread(lambda k: part_x.at[rank], part_x, rank, peer_x, half, pxs_sem, pxr_sem)
    for i in range(lx):
        work[row_x(i)] = local[i] - 2.0 * f_ref[row_x(i)]

    for i in range(lx):
        lo, hi, edge = faces_z(c_ref[row_x(i)])
        excess = 1.0 + edge
        shift, level = 1, 0
        while shift < depth:
            inverse = 1.0 / (excess + lo + hi)
            a = lo * pltpu.roll(inverse, shift, 1)
            b = hi * pltpu.roll(inverse, depth - shift, 1)
            pcr_lo[level, row_x(i)] = a
            pcr_hi[level, row_x(i)] = b
            excess = (excess + a * pltpu.roll(excess, shift, 1)
                      + b * pltpu.roll(excess, depth - shift, 1))
            lo = a * pltpu.roll(lo, shift, 1)
            hi = b * pltpu.roll(hi, depth - shift, 1)
            shift, level = 2 * shift, level + 1
        pcr_inv[row_x(i)] = 1.0 / (excess + lo + hi)

    for copy in mats_x:
        copy.wait()
    zeros = jnp.zeros_like(near)
    outer_x[0, 0] = zeros
    outer_x[1, 0] = zeros
    outer_x[2, 0] = zeros
    ratios = [zeros]
    joined = mat_x[0, 2]
    for q in range(1, half):
        link = 4.0 / (mat_x[q - 1, 4] + mat_x[q, 3])
        inverse = 1.0 / (link + joined + mat_x[q, 0])
        ratio = mat_x[q, 1] * inverse
        outer_x[0, q] = inverse
        outer_x[1, q] = ratio
        ratios.append(ratio)
        joined = mat_x[q, 2] - mat_x[q, 1] * ratio
    mid_out[0] = joined
    mid_out[1] = mat_x[half - 1, 4]
    mids = remote(mid_out, mid_in, mid_sem.at[0], mid_sem.at[1], mirror)

    for copy in mats_y:
        copy.wait()
    links = [4.0 / (mat_y[k, 4] + mat_y[k + 1, 3]) for k in range(ny - 1)]
    blank = jnp.zeros_like(links[0])
    alpha_y[0] = blank
    own_y[0, 0] = blank
    joined = mat_y[0, 2]
    for k in range(1, ny):
        inverse = 1.0 / (links[k - 1] + joined + mat_y[k, 0])
        ratio = mat_y[k, 1] * inverse
        alpha_y[k] = ratio
        own_y[0, k] = inverse
        joined = mat_y[k, 2] - mat_y[k, 1] * ratio
    beta_y[ny - 1] = blank
    own_y[1, ny - 1] = blank
    joined = mat_y[ny - 1, 0]
    for k in range(ny - 2, -1, -1):
        inverse = 1.0 / (links[k] + joined + mat_y[k, 2])
        ratio = mat_y[k, 1] * inverse
        beta_y[k] = ratio
        own_y[1, k] = inverse
        joined = mat_y[k, 0] - mat_y[k, 1] * ratio

    for copy in parts_x:
        copy.wait()
    before = part_x[0, 1]
    for q in range(1, half):
        outer_x[2, q] = before
        before = part_x[q, 1] + ratios[q] * (before - part_x[q, 0])
    chain_out[...] = before
    chained = remote(chain_out, chain_in, mid_sem.at[2], mid_sem.at[3], mirror)

    mids.wait()
    joined = mid_in[0]
    beyond = mid_in[1]
    ratios = [None] * half
    for q in range(half - 1, -1, -1):
        inverse = 1.0 / (4.0 / (mat_x[q, 4] + beyond) + joined + mat_x[q, 2])
        ratio = mat_x[q, 1] * inverse
        inner_x[0, q] = inverse
        inner_x[1, q] = ratio
        ratios[q] = ratio
        joined = mat_x[q, 0] - mat_x[q, 1] * ratio
        beyond = mat_x[q, 3]
    a, b = outer_x[1, rank], inner_x[1, rank]
    scale = 1.0 / (1.0 - a * b)
    gain_near = scale * outer_x[0, rank]
    gain_far = scale * inner_x[0, rank]
    left = outer_x[2, rank] - near
    chained.wait()
    after = chain_in[...]
    for q in range(half - 1, -1, -1):
        inner_x[2, q] = after
        if q:
            after = part_x[q, 0] + ratios[q] * (after - part_x[q, 1])
    right = far - inner_x[2, rank]
    into = gain_near * (left + b * right)
    out = gain_far * (right + a * left)
    on_head, on_tail = turn(into, -out)
    for i in range(lx):
        work[row_x(i)] += on_head * head_x[i] + on_tail * tail_x[i]

    local = substitute([work[row_y(j)] for j in range(ly)],
                       [None] + [mult_y[j] for j in range(1, ly)],
                       [inv_y[j] for j in range(ly)])
    head, tail = local[0], local[-1]
    a, b = alpha_y[iy], beta_y[iy]
    out_y[0] = tail - a * head
    out_y[1] = head - b * tail
    part_y[iy] = head
    copies = spread(lambda k: out_y.at[lax.div(iy + k, ny)], part_y, iy, peer_y, ny,
                    pys_sem, pyr_sem)
    for j in range(ly):
        work[row_y(j)] = local[j]
    scale = 1.0 / (1.0 - a * b)
    gain_in, gain_out = scale * own_y[0, iy], scale * own_y[1, iy]
    for copy in copies:
        copy.wait()
    before = blank
    for k in range(ny - 1):
        before = jnp.where(k < iy, alpha_y[k] * before + part_y[k], before)
    after = blank
    for k in range(ny - 1, 0, -1):
        after = jnp.where(k > iy, beta_y[k] * after + part_y[k], after)
    left = before - head
    right = tail - after
    into = gain_in * (left + b * right)
    out = gain_out * (right + a * left)
    for j in range(ly):
        work[row_y(j)] += into * head_y[j] - out * tail_y[j]

    shift, level = 1, 0
    right = work[...]
    while shift < depth:
        right = (right + pcr_lo[level] * pltpu.roll(right, shift, 1)
                 + pcr_hi[level] * pltpu.roll(right, depth - shift, 1))
        shift, level = 2 * shift, level + 1
    o_ref[...] = f_ref[...] + right * pcr_inv[...]


def solution(mesh):
    nx, ny = mesh.shape["gx"], mesh.shape["gy"]

    def body(field, conductance, source):
        lx, ly, depth = field.shape
        lines = lx * ly
        levels = max(1, (depth - 1).bit_length())
        f32 = jnp.float32

        def vmem(*shape):
            return pltpu.VMEM(shape, f32)

        def dma(count):
            return pltpu.SemaphoreType.DMA((count,))

        half = nx // 2
        along_x = [vmem(lx, ly, depth)] * 4
        along_y = [vmem(ly, lx, depth)] * 4
        out = pl.pallas_call(
            functools.partial(kernel, nx, ny, lx, ly, depth),
            out_shape=pltpu.VMEM((lines, depth), f32),
            in_specs=[pl.BlockSpec(memory_space=pltpu.HBM)] * 3,
            out_specs=pl.BlockSpec(memory_space=pltpu.VMEM),
            scratch_shapes=[vmem(lines, depth)] * 3 + along_x + along_y + [
                vmem(levels, lines, depth), vmem(levels, lines, depth), vmem(lines, depth),
                vmem(lines, depth), vmem(2, 2, lx, depth), vmem(2, 2, lx, depth),
                vmem(half, 5, ly, depth), vmem(ny, 5, lx, depth),
                vmem(3, half, ly, depth), vmem(3, half, ly, depth),
                vmem(ny, lx, depth), vmem(ny, lx, depth), vmem(2, ny, lx, depth),
                vmem(half, 2, ly, depth), vmem(ny, lx, depth), vmem(2, lx, depth),
                vmem(2, ly, depth), vmem(2, ly, depth), vmem(ly, depth), vmem(ly, depth),
                dma(3), dma(2), dma(2), dma(half - 1), dma(half - 1), dma(ny - 1), dma(ny - 1),
                dma(half - 1), dma(half - 1), dma(ny - 1), dma(ny - 1), dma(4),
            ],
            compiler_params=pltpu.CompilerParams(
                collective_id=0, has_side_effects=True),
            name="step",
        )(field.reshape(lines, depth), conductance.reshape(lines, depth),
          source.reshape(lines, depth))
        return out.reshape(lx, ly, depth)

    spec = P("gx", "gy", None)
    return jax.shard_map(body, mesh=mesh, in_specs=(spec, spec, spec), out_specs=spec,
                         check_vma=False)
```

```python
import functools

import jax
import jax.numpy as jnp
from jax import lax
from jax.experimental import pallas as pl
from jax.experimental.pallas import tpu as pltpu
from jax.sharding import PartitionSpec as P

MESH = pl.DeviceIdType.MESH


def factor(cells, first, last):
    count = len(cells)
    ones = jnp.ones_like(cells[0])
    excess = jnp.where(first, 1.0 + 0.25 * cells[0], ones)
    mults, inverses = [None], []
    for i in range(count):
        if i == count - 1:
            excess = excess + jnp.where(last, 0.25 * cells[i], 0.0)
            inverses.append(1.0 / excess)
        else:
            face = 0.25 * (cells[i] + cells[i + 1])
            inverse = 1.0 / (excess + face)
            mult = face * inverse
            inverses.append(inverse)
            mults.append(mult)
            excess = 1.0 + mult * excess
    from_last = [None] * count
    from_last[-1] = inverses[-1]
    for i in range(count - 2, -1, -1):
        from_last[i] = mults[i + 1] * from_last[i + 1]
    prods = [ones]
    for i in range(1, count):
        prods.append(mults[i] * prods[-1])
    from_first = [None] * count
    from_first[-1] = prods[-1] * inverses[-1]
    for i in range(count - 2, -1, -1):
        from_first[i] = prods[i] * inverses[i] + mults[i + 1] * from_first[i + 1]
    return mults, inverses, from_first, from_last


def substitute(rights, mults, inverses):
    count = len(rights)
    values = [rights[0]]
    for i in range(1, count):
        values.append(rights[i] + mults[i] * values[-1])
    out = [None] * count
    out[-1] = values[-1] * inverses[-1]
    for i in range(count - 2, -1, -1):
        out[i] = values[i] * inverses[i] + mults[i + 1] * out[i + 1]
    return out


def kernel(nx, ny, lx, ly, depth, f_hbm, c_hbm, s_hbm, o_ref,
           f_ref, c_ref, s_ref,
           mult_x, inv_x, head_x, tail_x, mult_y, inv_y, head_y, tail_y,
           pcr_lo, pcr_hi, pcr_inv, work, halo_out, halo_in,
           mat_x, mat_y, outer_x, inner_x, alpha_y, beta_y, own_y,
           part_x, part_y, out_y, mid_out, mid_in, chain_out, chain_in,
           edge_in, part_e, pes_sem, per_sem,
           in_sem, hs_sem, hr_sem, mxs_sem, mxr_sem, mys_sem, myr_sem,
           pxs_sem, pxr_sem, pys_sem, pyr_sem, mid_sem):
    ix = lax.axis_index("gx")
    iy = lax.axis_index("gy")
    half = nx // 2
    upper = lax.div(ix, half)
    place = ix - upper * half
    rank = ix + upper * (nx - 1 - 2 * ix)
    flip = upper == 1

    def peer_x(k):
        return (upper * half + lax.rem(place + k, half), iy)

    mirror = (lax.rem(ix + half, nx), iy)

    def peer_y(k):
        return (ix, lax.rem(iy + k, ny))

    barrier = pltpu.get_barrier_semaphore()
    pl.semaphore_signal(barrier, inc=1, device_id=mirror, device_id_type=MESH)
    for k in range(1, half):
        pl.semaphore_signal(barrier, inc=1, device_id=peer_x(k), device_id_type=MESH)
    for k in range(1, ny):
        pl.semaphore_signal(barrier, inc=1, device_id=peer_y(k), device_id_type=MESH)

    fetches = []
    for n, (src, dst) in enumerate(((c_hbm, c_ref), (f_hbm, f_ref), (s_hbm, s_ref))):
        fetch = pltpu.make_async_copy(src, dst, in_sem.at[n])
        fetch.start()
        fetches.append(fetch)

    def row_x(i):
        return pl.ds(i * ly, ly)

    def row_y(j):
        return pl.ds(j, lx, stride=ly)

    def keep(refs, lists):
        for ref, items in zip(refs, lists):
            for i, item in enumerate(items):
                if item is not None:
                    ref[i] = item

    def remote(src, dst, s_sem, r_sem, device):
        copy = pltpu.make_async_remote_copy(
            src_ref=src, dst_ref=dst, send_sem=s_sem, recv_sem=r_sem,
            device_id=device, device_id_type=MESH)
        copy.start()
        return copy

    def spread(src_of, table, index, peer, count, s_sem, r_sem):
        return [remote(src_of(k), table.at[index], s_sem.at[k - 1], r_sem.at[k - 1], peer(k))
                for k in range(1, count)]

    def turn(first, second):
        return jnp.where(flip, second, first), jnp.where(flip, first, second)

    fetches[0].wait()
    cells = [c_ref[row_x(i)] for i in range(lx)]
    parts = factor(cells, ix == 0, ix == nx - 1)
    keep((mult_x, inv_x, head_x, tail_x), parts)
    heads, tails = parts[2], parts[3]
    mat_x[rank, 0], mat_x[rank, 2] = turn(heads[0], tails[-1])
    mat_x[rank, 1] = tails[0]
    mat_x[rank, 3], mat_x[rank, 4] = turn(cells[0], cells[-1])
    fetches[1].wait()
    for side, j in ((0, 0), (1, ly - 1)):
        halo_out[side, 0] = f_ref[row_y(j)]
        halo_out[side, 1] = c_ref[row_y(j)]

    pl.semaphore_wait(barrier, half + ny - 1)

    halos = [remote(halo_out.at[side], halo_in.at[side], hs_sem.at[side], hr_sem.at[side],
                    peer_y(k)) for side, k in ((0, ny - 1), (1, 1))]
    mats_x = spread(lambda k: mat_x.at[rank], mat_x, rank, peer_x, half, mxs_sem, mxr_sem)

    cells = [c_ref[row_y(j)] for j in range(ly)]
    parts = factor(cells, iy == 0, iy == ny - 1)
    keep((mult_y, inv_y, head_y, tail_y), parts)
    heads, tails = parts[2], parts[3]
    mat_y[iy, 0] = heads[0]
    mat_y[iy, 1] = tails[0]
    mat_y[iy, 2] = tails[-1]
    mat_y[iy, 3] = cells[0]
    mat_y[iy, 4] = cells[-1]
    mats_y = spread(lambda k: mat_y.at[iy], mat_y, iy, peer_y, ny, mys_sem, myr_sem)

    lane = lax.broadcasted_iota(jnp.int32, (ly, depth), 1)
    low_end = lane == 0
    high_end = lane == depth - 1

    def faces_z(cond):
        lo = jnp.where(low_end, 0.0, 0.25 * (cond + pltpu.roll(cond, 1, 1)))
        hi = jnp.where(high_end, 0.0, 0.25 * (cond + pltpu.roll(cond, depth - 1, 1)))
        edge = jnp.where(low_end, 0.25 * cond, 0.0) + jnp.where(high_end, 0.25 * cond, 0.0)
        return lo, hi, edge

    fetches[2].wait()
    for i in range(lx):
        value = f_ref[row_x(i)]
        lo, hi, edge = faces_z(c_ref[row_x(i)])
        flux = (hi * (pltpu.roll(value, depth - 1, 1) - value)
                - lo * (value - pltpu.roll(value, 1, 1)) - edge * value)
        work[row_x(i)] = 2.0 * (value + flux) + s_ref[row_x(i)]

    value = f_ref[row_y(0)]
    cond = c_ref[row_y(0)]
    first_f, first_c = value, cond
    flux_lo = None
    for j in range(ly):
        if j == ly - 1:
            work[row_y(j)] += -flux_lo
            break
        next_f, next_c = f_ref[row_y(j + 1)], c_ref[row_y(j + 1)]
        flux_hi = 0.5 * (cond + next_c) * (next_f - value)
        work[row_y(j)] += flux_hi if flux_lo is None else flux_hi - flux_lo
        value, cond, flux_lo = next_f, next_c, flux_hi

    local = substitute([work[row_x(i)] for i in range(lx)],
                       [None] + [mult_x[i] for i in range(1, lx)],
                       [inv_x[i] for i in range(lx)])
    part_x[rank, 0], part_x[rank, 1] = turn(local[0], local[-1])
    parts_x = spread(lambda k: part_x.at[rank], part_x, rank, peer_x, half, pxs_sem, pxr_sem)
    for i in range(lx):
        work[row_x(i)] = local[i] - 2.0 * f_ref[row_x(i)]

    for copy in halos:
        copy.wait()
    below_f = jnp.where(iy == 0, 0.0, halo_in[1, 0])
    below_c = jnp.where(iy == 0, 0.0, halo_in[1, 1])
    above_f = jnp.where(iy == ny - 1, 0.0, halo_in[0, 0])
    above_c = jnp.where(iy == ny - 1, 0.0, halo_in[0, 1])
    edge_in[pl.ds(0, lx, stride=2)] = 0.5 * (below_c + first_c) * (below_f - first_f)
    edge_in[pl.ds(1, lx, stride=2)] = 0.5 * (cond + above_c) * (above_f - value)
    pair = pl.ds(0, 2, stride=ly - 1)
    local = substitute([edge_in[pl.ds(2 * i, 2)] for i in range(lx)],
                       [None] + [mult_x[i, pair] for i in range(1, lx)],
                       [inv_x[i, pair] for i in range(lx)])
    part_e[rank, 0], part_e[rank, 1] = turn(local[0], local[-1])
    parts_e = spread(lambda k: part_e.at[rank], part_e, rank, peer_x, half, pes_sem, per_sem)
    for i in range(lx):
        rows = pl.ds(i * ly, 2, stride=ly - 1)
        work[rows] = work[rows] + local[i]

    for i in range(lx):
        lo, hi, edge = faces_z(c_ref[row_x(i)])
        excess = 1.0 + edge
        shift, level = 1, 0
        while shift < depth:
            inverse = 1.0 / (excess + lo + hi)
            a = lo * pltpu.roll(inverse, shift, 1)
            b = hi * pltpu.roll(inverse, depth - shift, 1)
            pcr_lo[level, row_x(i)] = a
            pcr_hi[level, row_x(i)] = b
            excess = (excess + a * pltpu.roll(excess, shift, 1)
                      + b * pltpu.roll(excess, depth - shift, 1))
            lo = a * pltpu.roll(lo, shift, 1)
            hi = b * pltpu.roll(hi, depth - shift, 1)
            shift, level = 2 * shift, level + 1
        pcr_inv[row_x(i)] = 1.0 / (excess + lo + hi)

    for copy in mats_x:
        copy.wait()
    zeros = jnp.zeros_like(mat_x[0, 2])
    outer_x[0, 0] = zeros
    outer_x[1, 0] = zeros
    outer_x[2, 0] = zeros
    ratios = [zeros]
    joined = mat_x[0, 2]
    for q in range(1, half):
        link = 4.0 / (mat_x[q - 1, 4] + mat_x[q, 3])
        inverse = 1.0 / (link + joined + mat_x[q, 0])
        ratio = mat_x[q, 1] * inverse
        outer_x[0, q] = inverse
        outer_x[1, q] = ratio
        ratios.append(ratio)
        joined = mat_x[q, 2] - mat_x[q, 1] * ratio
    mid_out[0] = joined
    mid_out[1] = mat_x[half - 1, 4]
    mids = remote(mid_out, mid_in, mid_sem.at[0], mid_sem.at[1], mirror)

    for copy in mats_y:
        copy.wait()
    links = [4.0 / (mat_y[k, 4] + mat_y[k + 1, 3]) for k in range(ny - 1)]
    blank = jnp.zeros_like(links[0])
    alpha_y[0] = blank
    own_y[0, 0] = blank
    joined = mat_y[0, 2]
    for k in range(1, ny):
        inverse = 1.0 / (links[k - 1] + joined + mat_y[k, 0])
        ratio = mat_y[k, 1] * inverse
        alpha_y[k] = ratio
        own_y[0, k] = inverse
        joined = mat_y[k, 2] - mat_y[k, 1] * ratio
    beta_y[ny - 1] = blank
    own_y[1, ny - 1] = blank
    joined = mat_y[ny - 1, 0]
    for k in range(ny - 2, -1, -1):
        inverse = 1.0 / (links[k] + joined + mat_y[k, 2])
        ratio = mat_y[k, 1] * inverse
        beta_y[k] = ratio
        own_y[1, k] = inverse
        joined = mat_y[k, 0] - mat_y[k, 1] * ratio

    for copy in parts_x + parts_e:
        copy.wait()
    for q in range(half):
        for side in range(2):
            part_x[q, side, pair] = part_x[q, side, pair] + part_e[q, side]
    near, far = part_x[rank, 0], part_x[rank, 1]
    before = part_x[0, 1]
    for q in range(1, half):
        outer_x[2, q] = before
        before = part_x[q, 1] + ratios[q] * (before - part_x[q, 0])
    chain_out[...] = before
    chained = remote(chain_out, chain_in, mid_sem.at[2], mid_sem.at[3], mirror)

    mids.wait()
    joined = mid_in[0]
    beyond = mid_in[1]
    ratios = [None] * half
    for q in range(half - 1, -1, -1):
        inverse = 1.0 / (4.0 / (mat_x[q, 4] + beyond) + joined + mat_x[q, 2])
        ratio = mat_x[q, 1] * inverse
        inner_x[0, q] = inverse
        inner_x[1, q] = ratio
        ratios[q] = ratio
        joined = mat_x[q, 0] - mat_x[q, 1] * ratio
        beyond = mat_x[q, 3]
    a, b = outer_x[1, rank], inner_x[1, rank]
    scale = 1.0 / (1.0 - a * b)
    gain_near = scale * outer_x[0, rank]
    gain_far = scale * inner_x[0, rank]
    left = outer_x[2, rank] - near
    chained.wait()
    after = chain_in[...]
    for q in range(half - 1, -1, -1):
        inner_x[2, q] = after
        if q:
            after = part_x[q, 0] + ratios[q] * (after - part_x[q, 1])
    right = far - inner_x[2, rank]
    into = gain_near * (left + b * right)
    out = gain_far * (right + a * left)
    on_head, on_tail = turn(into, -out)
    for i in range(lx):
        work[row_x(i)] += on_head * head_x[i] + on_tail * tail_x[i]

    local = substitute([work[row_y(j)] for j in range(ly)],
                       [None] + [mult_y[j] for j in range(1, ly)],
                       [inv_y[j] for j in range(ly)])
    head, tail = local[0], local[-1]
    a, b = alpha_y[iy], beta_y[iy]
    out_y[0] = tail - a * head
    out_y[1] = head - b * tail
    part_y[iy] = head
    copies = spread(lambda k: out_y.at[lax.div(iy + k, ny)], part_y, iy, peer_y, ny,
                    pys_sem, pyr_sem)
    for j in range(ly):
        work[row_y(j)] = local[j]
    scale = 1.0 / (1.0 - a * b)
    gain_in, gain_out = scale * own_y[0, iy], scale * own_y[1, iy]
    for copy in copies:
        copy.wait()
    before = blank
    for k in range(ny - 1):
        before = jnp.where(k < iy, alpha_y[k] * before + part_y[k], before)
    after = blank
    for k in range(ny - 1, 0, -1):
        after = jnp.where(k > iy, beta_y[k] * after + part_y[k], after)
    left = before - head
    right = tail - after
    into = gain_in * (left + b * right)
    out = gain_out * (right + a * left)
    for j in range(ly):
        work[row_y(j)] += into * head_y[j] - out * tail_y[j]

    shift, level = 1, 0
    right = work[...]
    while shift < depth:
        right = (right + pcr_lo[level] * pltpu.roll(right, shift, 1)
                 + pcr_hi[level] * pltpu.roll(right, depth - shift, 1))
        shift, level = 2 * shift, level + 1
    o_ref[...] = f_ref[...] + right * pcr_inv[...]


def solution(mesh):
    nx, ny = mesh.shape["gx"], mesh.shape["gy"]

    def body(field, conductance, source):
        lx, ly, depth = field.shape
        lines = lx * ly
        levels = max(1, (depth - 1).bit_length())
        f32 = jnp.float32

        def vmem(*shape):
            return pltpu.VMEM(shape, f32)

        def dma(count):
            return pltpu.SemaphoreType.DMA((count,))

        half = nx // 2
        along_x = [vmem(lx, ly, depth)] * 4
        along_y = [vmem(ly, lx, depth)] * 4
        out = pl.pallas_call(
            functools.partial(kernel, nx, ny, lx, ly, depth),
            out_shape=pltpu.VMEM((lines, depth), f32),
            in_specs=[pl.BlockSpec(memory_space=pltpu.HBM)] * 3,
            out_specs=pl.BlockSpec(memory_space=pltpu.VMEM),
            scratch_shapes=[vmem(lines, depth)] * 3 + along_x + along_y + [
                vmem(levels, lines, depth), vmem(levels, lines, depth), vmem(lines, depth),
                vmem(lines, depth), vmem(2, 2, lx, depth), vmem(2, 2, lx, depth),
                vmem(half, 5, ly, depth), vmem(ny, 5, lx, depth),
                vmem(3, half, ly, depth), vmem(3, half, ly, depth),
                vmem(ny, lx, depth), vmem(ny, lx, depth), vmem(2, ny, lx, depth),
                vmem(half, 2, ly, depth), vmem(ny, lx, depth), vmem(2, lx, depth),
                vmem(2, ly, depth), vmem(2, ly, depth), vmem(ly, depth), vmem(ly, depth),
                vmem(2 * lx, depth), vmem(half, 2, 2, depth), dma(half - 1), dma(half - 1),
                dma(3), dma(2), dma(2), dma(half - 1), dma(half - 1), dma(ny - 1), dma(ny - 1),
                dma(half - 1), dma(half - 1), dma(ny - 1), dma(ny - 1), dma(4),
            ],
            compiler_params=pltpu.CompilerParams(
                collective_id=0, has_side_effects=True),
            name="step",
        )(field.reshape(lines, depth), conductance.reshape(lines, depth),
          source.reshape(lines, depth))
        return out.reshape(lx, ly, depth)

    spec = P("gx", "gy", None)
    return jax.shard_map(body, mesh=mesh, in_specs=(spec, spec, spec), out_specs=spec,
                         check_vma=False)
```

```python
import functools

import jax
import jax.numpy as jnp
from jax import lax
from jax.experimental import pallas as pl
from jax.experimental.pallas import tpu as pltpu
from jax.sharding import PartitionSpec as P

MESH = pl.DeviceIdType.MESH


def factor(cells, first, last):
    count = len(cells)
    ones = jnp.ones_like(cells[0])
    excess = jnp.where(first, 1.0 + 0.25 * cells[0], ones)
    mults, inverses = [None], []
    for i in range(count):
        if i == count - 1:
            excess = excess + jnp.where(last, 0.25 * cells[i], 0.0)
            inverses.append(1.0 / excess)
        else:
            face = 0.25 * (cells[i] + cells[i + 1])
            inverse = 1.0 / (excess + face)
            mult = face * inverse
            inverses.append(inverse)
            mults.append(mult)
            excess = 1.0 + mult * excess
    from_last = [None] * count
    from_last[-1] = inverses[-1]
    for i in range(count - 2, -1, -1):
        from_last[i] = mults[i + 1] * from_last[i + 1]
    prods = [ones]
    for i in range(1, count):
        prods.append(mults[i] * prods[-1])
    from_first = [None] * count
    from_first[-1] = prods[-1] * inverses[-1]
    for i in range(count - 2, -1, -1):
        from_first[i] = prods[i] * inverses[i] + mults[i + 1] * from_first[i + 1]
    return mults, inverses, from_first, from_last


def substitute(rights, mults, inverses):
    count = len(rights)
    values = [rights[0]]
    for i in range(1, count):
        values.append(rights[i] + mults[i] * values[-1])
    out = [None] * count
    out[-1] = values[-1] * inverses[-1]
    for i in range(count - 2, -1, -1):
        out[i] = values[i] * inverses[i] + mults[i + 1] * out[i + 1]
    return out


def kernel(nx, ny, lx, ly, depth, f_hbm, c_hbm, s_hbm, o_ref,
           f_ref, c_ref, s_ref,
           mult_x, inv_x, head_x, tail_x, mult_y, inv_y, head_y, tail_y,
           pcr_lo, pcr_hi, pcr_inv, work, halo_out, halo_in,
           mat_x, mat_y, outer_x, inner_x, alpha_y, beta_y, own_y,
           part_x, part_y, out_y, mid_out, mid_in, chain_out, chain_in,
           edge_in, part_e, pes_sem, per_sem,
           in_sem, hs_sem, hr_sem, mxs_sem, mxr_sem, mys_sem, myr_sem,
           pxs_sem, pxr_sem, pys_sem, pyr_sem, mid_sem):
    ix = lax.axis_index("gx")
    iy = lax.axis_index("gy")
    half = nx // 2
    upper = lax.div(ix, half)
    place = ix - upper * half
    rank = ix + upper * (nx - 1 - 2 * ix)
    flip = upper == 1

    def peer_x(k):
        return (upper * half + lax.rem(place + k, half), iy)

    mirror = (lax.rem(ix + half, nx), iy)

    def peer_y(k):
        return (ix, lax.rem(iy + k, ny))

    barrier = pltpu.get_barrier_semaphore()
    pl.semaphore_signal(barrier, inc=1, device_id=mirror, device_id_type=MESH)
    for k in range(1, half):
        pl.semaphore_signal(barrier, inc=1, device_id=peer_x(k), device_id_type=MESH)
    for k in range(1, ny):
        pl.semaphore_signal(barrier, inc=1, device_id=peer_y(k), device_id_type=MESH)

    fetches = []
    for n, (src, dst) in enumerate(((c_hbm, c_ref), (f_hbm, f_ref), (s_hbm, s_ref))):
        fetch = pltpu.make_async_copy(src, dst, in_sem.at[n])
        fetch.start()
        fetches.append(fetch)

    def row_x(i):
        return pl.ds(i * ly, ly)

    def row_y(j):
        return pl.ds(j, lx, stride=ly)

    def keep(refs, lists):
        for ref, items in zip(refs, lists):
            for i, item in enumerate(items):
                if item is not None:
                    ref[i] = item

    def remote(src, dst, s_sem, r_sem, device):
        copy = pltpu.make_async_remote_copy(
            src_ref=src, dst_ref=dst, send_sem=s_sem, recv_sem=r_sem,
            device_id=device, device_id_type=MESH)
        copy.start()
        return copy

    def spread(src_of, table, index, peer, count, s_sem, r_sem):
        return [remote(src_of(k), table.at[index], s_sem.at[k - 1], r_sem.at[k - 1], peer(k))
                for k in range(1, count)]

    def turn(first, second):
        return jnp.where(flip, second, first), jnp.where(flip, first, second)

    fetches[0].wait()
    cells = [c_ref[row_x(i)] for i in range(lx)]
    parts = factor(cells, ix == 0, ix == nx - 1)
    keep((mult_x, inv_x, head_x, tail_x), parts)
    heads, tails = parts[2], parts[3]
    mat_x[rank, 0], mat_x[rank, 2] = turn(heads[0], tails[-1])
    mat_x[rank, 1] = tails[0]
    mat_x[rank, 3], mat_x[rank, 4] = turn(cells[0], cells[-1])
    fetches[1].wait()
    for side, j in ((0, 0), (1, ly - 1)):
        halo_out[side, 0] = f_ref[row_y(j)]
        halo_out[side, 1] = c_ref[row_y(j)]

    pl.semaphore_wait(barrier, half + ny - 1)

    halos = [remote(halo_out.at[side], halo_in.at[side], hs_sem.at[side], hr_sem.at[side],
                    peer_y(k)) for side, k in ((0, ny - 1), (1, 1))]
    mats_x = spread(lambda k: mat_x.at[rank], mat_x, rank, peer_x, half, mxs_sem, mxr_sem)

    cells = [c_ref[row_y(j)] for j in range(ly)]
    parts = factor(cells, iy == 0, iy == ny - 1)
    keep((mult_y, inv_y, head_y, tail_y), parts)
    heads, tails = parts[2], parts[3]
    mat_y[iy, 0] = heads[0]
    mat_y[iy, 1] = tails[0]
    mat_y[iy, 2] = tails[-1]
    mat_y[iy, 3] = cells[0]
    mat_y[iy, 4] = cells[-1]
    mats_y = spread(lambda k: mat_y.at[iy], mat_y, iy, peer_y, ny, mys_sem, myr_sem)

    lane = lax.broadcasted_iota(jnp.int32, (ly, depth), 1)
    low_end = lane == 0
    high_end = lane == depth - 1

    def faces_z(cond):
        lo = jnp.where(low_end, 0.0, 0.25 * (cond + pltpu.roll(cond, 1, 1)))
        hi = jnp.where(high_end, 0.0, 0.25 * (cond + pltpu.roll(cond, depth - 1, 1)))
        edge = jnp.where(low_end, 0.25 * cond, 0.0) + jnp.where(high_end, 0.25 * cond, 0.0)
        return lo, hi, edge

    fetches[2].wait()
    for i in range(lx):
        value = f_ref[row_x(i)]
        lo, hi, edge = faces_z(c_ref[row_x(i)])
        flux = (hi * (pltpu.roll(value, depth - 1, 1) - value)
                - lo * (value - pltpu.roll(value, 1, 1)) - edge * value)
        work[row_x(i)] = 2.0 * (value + flux) + s_ref[row_x(i)]

    value = f_ref[row_y(0)]
    cond = c_ref[row_y(0)]
    first_f, first_c = value, cond
    flux_lo = None
    for j in range(ly):
        if j == ly - 1:
            work[row_y(j)] += -flux_lo
            break
        next_f, next_c = f_ref[row_y(j + 1)], c_ref[row_y(j + 1)]
        flux_hi = 0.5 * (cond + next_c) * (next_f - value)
        work[row_y(j)] += flux_hi if flux_lo is None else flux_hi - flux_lo
        value, cond, flux_lo = next_f, next_c, flux_hi

    local = substitute([work[row_x(i)] for i in range(lx)],
                       [None] + [mult_x[i] for i in range(1, lx)],
                       [inv_x[i] for i in range(lx)])
    part_x[rank, 0], part_x[rank, 1] = turn(local[0], local[-1])
    parts_x = spread(lambda k: part_x.at[rank], part_x, rank, peer_x, half, pxs_sem, pxr_sem)
    for i in range(lx):
        work[row_x(i)] = local[i] - 2.0 * f_ref[row_x(i)]

    for i in range(lx):
        lo, hi, edge = faces_z(c_ref[row_x(i)])
        excess = 1.0 + edge
        shift, level = 1, 0
        while shift < depth:
            inverse = 1.0 / (excess + lo + hi)
            a = lo * pltpu.roll(inverse, shift, 1)
            b = hi * pltpu.roll(inverse, depth - shift, 1)
            pcr_lo[level, row_x(i)] = a
            pcr_hi[level, row_x(i)] = b
            excess = (excess + a * pltpu.roll(excess, shift, 1)
                      + b * pltpu.roll(excess, depth - shift, 1))
            lo = a * pltpu.roll(lo, shift, 1)
            hi = b * pltpu.roll(hi, depth - shift, 1)
            shift, level = 2 * shift, level + 1
        pcr_inv[row_x(i)] = 1.0 / (excess + lo + hi)

    for copy in halos:
        copy.wait()
    below_f = jnp.where(iy == 0, 0.0, halo_in[1, 0])
    below_c = jnp.where(iy == 0, 0.0, halo_in[1, 1])
    above_f = jnp.where(iy == ny - 1, 0.0, halo_in[0, 0])
    above_c = jnp.where(iy == ny - 1, 0.0, halo_in[0, 1])
    edge_in[pl.ds(0, lx, stride=2)] = 0.5 * (below_c + first_c) * (below_f - first_f)
    edge_in[pl.ds(1, lx, stride=2)] = 0.5 * (cond + above_c) * (above_f - value)
    pair = pl.ds(0, 2, stride=ly - 1)
    local = substitute([edge_in[pl.ds(2 * i, 2)] for i in range(lx)],
                       [None] + [mult_x[i, pair] for i in range(1, lx)],
                       [inv_x[i, pair] for i in range(lx)])
    part_e[rank, 0], part_e[rank, 1] = turn(local[0], local[-1])
    parts_e = spread(lambda k: part_e.at[rank], part_e, rank, peer_x, half, pes_sem, per_sem)
    for i in range(lx):
        rows = pl.ds(i * ly, 2, stride=ly - 1)
        work[rows] = work[rows] + local[i]

    for copy in mats_x:
        copy.wait()
    zeros = jnp.zeros_like(mat_x[0, 2])
    outer_x[0, 0] = zeros
    outer_x[1, 0] = zeros
    outer_x[2, 0] = zeros
    ratios = [zeros]
    joined = mat_x[0, 2]
    for q in range(1, half):
        link = 4.0 / (mat_x[q - 1, 4] + mat_x[q, 3])
        inverse = 1.0 / (link + joined + mat_x[q, 0])
        ratio = mat_x[q, 1] * inverse
        outer_x[0, q] = inverse
        outer_x[1, q] = ratio
        ratios.append(ratio)
        joined = mat_x[q, 2] - mat_x[q, 1] * ratio
    mid_out[0] = joined
    mid_out[1] = mat_x[half - 1, 4]
    mids = remote(mid_out, mid_in, mid_sem.at[0], mid_sem.at[1], mirror)

    for copy in mats_y:
        copy.wait()
    links = [4.0 / (mat_y[k, 4] + mat_y[k + 1, 3]) for k in range(ny - 1)]
    blank = jnp.zeros_like(links[0])
    alpha_y[0] = blank
    own_y[0, 0] = blank
    joined = mat_y[0, 2]
    for k in range(1, ny):
        inverse = 1.0 / (links[k - 1] + joined + mat_y[k, 0])
        ratio = mat_y[k, 1] * inverse
        alpha_y[k] = ratio
        own_y[0, k] = inverse
        joined = mat_y[k, 2] - mat_y[k, 1] * ratio
    beta_y[ny - 1] = blank
    own_y[1, ny - 1] = blank
    joined = mat_y[ny - 1, 0]
    for k in range(ny - 2, -1, -1):
        inverse = 1.0 / (links[k] + joined + mat_y[k, 2])
        ratio = mat_y[k, 1] * inverse
        beta_y[k] = ratio
        own_y[1, k] = inverse
        joined = mat_y[k, 0] - mat_y[k, 1] * ratio

    for copy in parts_x + parts_e:
        copy.wait()
    for q in range(half):
        for side in range(2):
            part_x[q, side, pair] = part_x[q, side, pair] + part_e[q, side]
    near, far = part_x[rank, 0], part_x[rank, 1]
    before = part_x[0, 1]
    for q in range(1, half):
        outer_x[2, q] = before
        before = part_x[q, 1] + ratios[q] * (before - part_x[q, 0])
    chain_out[...] = before
    chained = remote(chain_out, chain_in, mid_sem.at[2], mid_sem.at[3], mirror)

    mids.wait()
    joined = mid_in[0]
    beyond = mid_in[1]
    ratios = [None] * half
    for q in range(half - 1, -1, -1):
        inverse = 1.0 / (4.0 / (mat_x[q, 4] + beyond) + joined + mat_x[q, 2])
        ratio = mat_x[q, 1] * inverse
        inner_x[0, q] = inverse
        inner_x[1, q] = ratio
        ratios[q] = ratio
        joined = mat_x[q, 0] - mat_x[q, 1] * ratio
        beyond = mat_x[q, 3]
    a, b = outer_x[1, rank], inner_x[1, rank]
    scale = 1.0 / (1.0 - a * b)
    gain_near = scale * outer_x[0, rank]
    gain_far = scale * inner_x[0, rank]
    left = outer_x[2, rank] - near
    chained.wait()
    after = chain_in[...]
    for q in range(half - 1, -1, -1):
        inner_x[2, q] = after
        if q:
            after = part_x[q, 0] + ratios[q] * (after - part_x[q, 1])
    right = far - inner_x[2, rank]
    into = gain_near * (left + b * right)
    out = gain_far * (right + a * left)
    on_head, on_tail = turn(into, -out)
    for i in range(lx):
        work[row_x(i)] += on_head * head_x[i] + on_tail * tail_x[i]

    local = substitute([work[row_y(j)] for j in range(ly)],
                       [None] + [mult_y[j] for j in range(1, ly)],
                       [inv_y[j] for j in range(ly)])
    head, tail = local[0], local[-1]
    a, b = alpha_y[iy], beta_y[iy]
    out_y[0] = tail - a * head
    out_y[1] = head - b * tail
    part_y[iy] = head
    copies = spread(lambda k: out_y.at[lax.div(iy + k, ny)], part_y, iy, peer_y, ny,
                    pys_sem, pyr_sem)
    for j in range(ly):
        work[row_y(j)] = local[j]
    scale = 1.0 / (1.0 - a * b)
    gain_in, gain_out = scale * own_y[0, iy], scale * own_y[1, iy]
    for copy in copies:
        copy.wait()
    before = blank
    for k in range(ny - 1):
        before = jnp.where(k < iy, alpha_y[k] * before + part_y[k], before)
    after = blank
    for k in range(ny - 1, 0, -1):
        after = jnp.where(k > iy, beta_y[k] * after + part_y[k], after)
    left = before - head
    right = tail - after
    into = gain_in * (left + b * right)
    out = gain_out * (right + a * left)
    for j in range(ly):
        work[row_y(j)] += into * head_y[j] - out * tail_y[j]

    shift, level = 1, 0
    right = work[...]
    while shift < depth:
        right = (right + pcr_lo[level] * pltpu.roll(right, shift, 1)
                 + pcr_hi[level] * pltpu.roll(right, depth - shift, 1))
        shift, level = 2 * shift, level + 1
    o_ref[...] = f_ref[...] + right * pcr_inv[...]


def solution(mesh):
    nx, ny = mesh.shape["gx"], mesh.shape["gy"]

    def body(field, conductance, source):
        lx, ly, depth = field.shape
        lines = lx * ly
        levels = max(1, (depth - 1).bit_length())
        f32 = jnp.float32

        def vmem(*shape):
            return pltpu.VMEM(shape, f32)

        def dma(count):
            return pltpu.SemaphoreType.DMA((count,))

        half = nx // 2
        along_x = [vmem(lx, ly, depth)] * 4
        along_y = [vmem(ly, lx, depth)] * 4
        out = pl.pallas_call(
            functools.partial(kernel, nx, ny, lx, ly, depth),
            out_shape=pltpu.VMEM((lines, depth), f32),
            in_specs=[pl.BlockSpec(memory_space=pltpu.HBM)] * 3,
            out_specs=pl.BlockSpec(memory_space=pltpu.VMEM),
            scratch_shapes=[vmem(lines, depth)] * 3 + along_x + along_y + [
                vmem(levels, lines, depth), vmem(levels, lines, depth), vmem(lines, depth),
                vmem(lines, depth), vmem(2, 2, lx, depth), vmem(2, 2, lx, depth),
                vmem(half, 5, ly, depth), vmem(ny, 5, lx, depth),
                vmem(3, half, ly, depth), vmem(3, half, ly, depth),
                vmem(ny, lx, depth), vmem(ny, lx, depth), vmem(2, ny, lx, depth),
                vmem(half, 2, ly, depth), vmem(ny, lx, depth), vmem(2, lx, depth),
                vmem(2, ly, depth), vmem(2, ly, depth), vmem(ly, depth), vmem(ly, depth),
                vmem(2 * lx, depth), vmem(half, 2, 2, depth), dma(half - 1), dma(half - 1),
                dma(3), dma(2), dma(2), dma(half - 1), dma(half - 1), dma(ny - 1), dma(ny - 1),
                dma(half - 1), dma(half - 1), dma(ny - 1), dma(ny - 1), dma(4),
            ],
            compiler_params=pltpu.CompilerParams(
                collective_id=0, has_side_effects=True),
            name="step",
        )(field.reshape(lines, depth), conductance.reshape(lines, depth),
          source.reshape(lines, depth))
        return out.reshape(lx, ly, depth)

    spec = P("gx", "gy", None)
    return jax.shard_map(body, mesh=mesh, in_specs=(spec, spec, spec), out_specs=spec,
                         check_vma=False)
```

```python
import functools

import jax
import jax.numpy as jnp
from jax import lax
from jax.experimental import pallas as pl
from jax.experimental.pallas import tpu as pltpu
from jax.sharding import PartitionSpec as P

MESH = pl.DeviceIdType.MESH


def factor(cells, first, last):
    count = len(cells)
    ones = jnp.ones_like(cells[0])
    excess = jnp.where(first, 1.0 + 0.25 * cells[0], ones)
    mults, inverses = [None], []
    for i in range(count):
        if i == count - 1:
            excess = excess + jnp.where(last, 0.25 * cells[i], 0.0)
            inverses.append(1.0 / excess)
        else:
            face = 0.25 * (cells[i] + cells[i + 1])
            inverse = 1.0 / (excess + face)
            mult = face * inverse
            inverses.append(inverse)
            mults.append(mult)
            excess = 1.0 + mult * excess
    from_last = [None] * count
    from_last[-1] = inverses[-1]
    for i in range(count - 2, -1, -1):
        from_last[i] = mults[i + 1] * from_last[i + 1]
    prods = [ones]
    for i in range(1, count):
        prods.append(mults[i] * prods[-1])
    from_first = [None] * count
    from_first[-1] = prods[-1] * inverses[-1]
    for i in range(count - 2, -1, -1):
        from_first[i] = prods[i] * inverses[i] + mults[i + 1] * from_first[i + 1]
    return mults, inverses, from_first, from_last


def substitute(rights, mults, inverses):
    count = len(rights)
    values = [rights[0]]
    for i in range(1, count):
        values.append(rights[i] + mults[i] * values[-1])
    out = [None] * count
    out[-1] = values[-1] * inverses[-1]
    for i in range(count - 2, -1, -1):
        out[i] = values[i] * inverses[i] + mults[i + 1] * out[i + 1]
    return out


def kernel(nx, ny, lx, ly, depth, f_hbm, c_hbm, s_hbm, o_ref,
           f_ref, c_ref, s_ref,
           mult_x, inv_x, head_x, tail_x, mult_y, inv_y, head_y, tail_y,
           pcr_lo, pcr_hi, pcr_inv, work, halo_out, halo_in,
           mat_x, mat_y, outer_x, inner_x, alpha_y, beta_y, own_y,
           part_x, part_y, out_y, mid_out, mid_in, chain_out, chain_in,
           edge_in, part_e, pes_sem, per_sem,
           in_sem, hs_sem, hr_sem, mxs_sem, mxr_sem, mys_sem, myr_sem,
           pxs_sem, pxr_sem, pys_sem, pyr_sem, mid_sem):
    ix = lax.axis_index("gx")
    iy = lax.axis_index("gy")
    half = nx // 2
    upper = lax.div(ix, half)
    place = ix - upper * half
    rank = ix + upper * (nx - 1 - 2 * ix)
    flip = upper == 1

    def peer_x(k):
        return (upper * half + lax.rem(place + k, half), iy)

    mirror = (lax.rem(ix + half, nx), iy)

    def peer_y(k):
        return (ix, lax.rem(iy + k, ny))

    barrier = pltpu.get_barrier_semaphore()
    pl.semaphore_signal(barrier, inc=1, device_id=mirror, device_id_type=MESH)
    for k in range(1, half):
        pl.semaphore_signal(barrier, inc=1, device_id=peer_x(k), device_id_type=MESH)
    for k in range(1, ny):
        pl.semaphore_signal(barrier, inc=1, device_id=peer_y(k), device_id_type=MESH)

    fetches = []
    for n, (src, dst) in enumerate(((c_hbm, c_ref), (f_hbm, f_ref), (s_hbm, s_ref))):
        fetch = pltpu.make_async_copy(src, dst, in_sem.at[n])
        fetch.start()
        fetches.append(fetch)

    def row_x(i):
        return pl.ds(i * ly, ly)

    def row_y(j):
        return pl.ds(j, lx, stride=ly)

    def keep(refs, lists):
        for ref, items in zip(refs, lists):
            for i, item in enumerate(items):
                if item is not None:
                    ref[i] = item

    def remote(src, dst, s_sem, r_sem, device):
        copy = pltpu.make_async_remote_copy(
            src_ref=src, dst_ref=dst, send_sem=s_sem, recv_sem=r_sem,
            device_id=device, device_id_type=MESH)
        copy.start()
        return copy

    def spread(src_of, table, index, peer, count, s_sem, r_sem):
        return [remote(src_of(k), table.at[index], s_sem.at[k - 1], r_sem.at[k - 1], peer(k))
                for k in range(1, count)]

    def turn(first, second):
        return jnp.where(flip, second, first), jnp.where(flip, first, second)

    fetches[0].wait()
    cells = [c_ref[row_x(i)] for i in range(lx)]
    parts = factor(cells, ix == 0, ix == nx - 1)
    keep((mult_x, inv_x, head_x, tail_x), parts)
    heads, tails = parts[2], parts[3]
    mat_x[rank, 0], mat_x[rank, 2] = turn(heads[0], tails[-1])
    mat_x[rank, 1] = tails[0]
    mat_x[rank, 3], mat_x[rank, 4] = turn(cells[0], cells[-1])
    fetches[1].wait()
    for side, j in ((0, 0), (1, ly - 1)):
        halo_out[side, 0] = f_ref[row_y(j)]
        halo_out[side, 1] = c_ref[row_y(j)]

    pl.semaphore_wait(barrier, half + ny - 1)

    halos = [remote(halo_out.at[side], halo_in.at[side], hs_sem.at[side], hr_sem.at[side],
                    peer_y(k)) for side, k in ((0, ny - 1), (1, 1))]
    mats_x = spread(lambda k: mat_x.at[rank], mat_x, rank, peer_x, half, mxs_sem, mxr_sem)

    cells = [c_ref[row_y(j)] for j in range(ly)]
    parts = factor(cells, iy == 0, iy == ny - 1)
    keep((mult_y, inv_y, head_y, tail_y), parts)
    heads, tails = parts[2], parts[3]
    mat_y[iy, 0] = heads[0]
    mat_y[iy, 1] = tails[0]
    mat_y[iy, 2] = tails[-1]
    mat_y[iy, 3] = cells[0]
    mat_y[iy, 4] = cells[-1]
    mats_y = spread(lambda k: mat_y.at[iy], mat_y, iy, peer_y, ny, mys_sem, myr_sem)

    lane = lax.broadcasted_iota(jnp.int32, (ly, depth), 1)
    low_end = lane == 0
    high_end = lane == depth - 1

    def faces_z(cond):
        lo = jnp.where(low_end, 0.0, 0.25 * (cond + pltpu.roll(cond, 1, 1)))
        hi = jnp.where(high_end, 0.0, 0.25 * (cond + pltpu.roll(cond, depth - 1, 1)))
        edge = jnp.where(low_end, 0.25 * cond, 0.0) + jnp.where(high_end, 0.25 * cond, 0.0)
        return lo, hi, edge

    def factor_z(start, stop):
        for i in range(start, stop):
            lo, hi, edge = faces_z(c_ref[row_x(i)])
            excess = 1.0 + edge
            shift, level = 1, 0
            while shift < depth:
                inverse = 1.0 / (excess + lo + hi)
                a = lo * pltpu.roll(inverse, shift, 1)
                b = hi * pltpu.roll(inverse, depth - shift, 1)
                pcr_lo[level, row_x(i)] = a
                pcr_hi[level, row_x(i)] = b
                excess = (excess + a * pltpu.roll(excess, shift, 1)
                          + b * pltpu.roll(excess, depth - shift, 1))
                lo = a * pltpu.roll(lo, shift, 1)
                hi = b * pltpu.roll(hi, depth - shift, 1)
                shift, level = 2 * shift, level + 1
            pcr_inv[row_x(i)] = 1.0 / (excess + lo + hi)

    fetches[2].wait()
    for i in range(lx):
        value = f_ref[row_x(i)]
        lo, hi, edge = faces_z(c_ref[row_x(i)])
        flux = (hi * (pltpu.roll(value, depth - 1, 1) - value)
                - lo * (value - pltpu.roll(value, 1, 1)) - edge * value)
        work[row_x(i)] = 2.0 * (value + flux) + s_ref[row_x(i)]

    value = f_ref[row_y(0)]
    cond = c_ref[row_y(0)]
    first_f, first_c = value, cond
    flux_lo = None
    for j in range(ly):
        if j == ly - 1:
            work[row_y(j)] += -flux_lo
            break
        next_f, next_c = f_ref[row_y(j + 1)], c_ref[row_y(j + 1)]
        flux_hi = 0.5 * (cond + next_c) * (next_f - value)
        work[row_y(j)] += flux_hi if flux_lo is None else flux_hi - flux_lo
        value, cond, flux_lo = next_f, next_c, flux_hi

    local = substitute([work[row_x(i)] for i in range(lx)],
                       [None] + [mult_x[i] for i in range(1, lx)],
                       [inv_x[i] for i in range(lx)])
    part_x[rank, 0], part_x[rank, 1] = turn(local[0], local[-1])
    parts_x = spread(lambda k: part_x.at[rank], part_x, rank, peer_x, half, pxs_sem, pxr_sem)
    for i in range(lx):
        work[row_x(i)] = local[i] - 2.0 * f_ref[row_x(i)]

    for copy in halos:
        copy.wait()
    below_f = jnp.where(iy == 0, 0.0, halo_in[1, 0])
    below_c = jnp.where(iy == 0, 0.0, halo_in[1, 1])
    above_f = jnp.where(iy == ny - 1, 0.0, halo_in[0, 0])
    above_c = jnp.where(iy == ny - 1, 0.0, halo_in[0, 1])
    edge_in[pl.ds(0, lx, stride=2)] = 0.5 * (below_c + first_c) * (below_f - first_f)
    edge_in[pl.ds(1, lx, stride=2)] = 0.5 * (cond + above_c) * (above_f - value)
    pair = pl.ds(0, 2, stride=ly - 1)
    local = substitute([edge_in[pl.ds(2 * i, 2)] for i in range(lx)],
                       [None] + [mult_x[i, pair] for i in range(1, lx)],
                       [inv_x[i, pair] for i in range(lx)])
    part_e[rank, 0], part_e[rank, 1] = turn(local[0], local[-1])
    parts_e = spread(lambda k: part_e.at[rank], part_e, rank, peer_x, half, pes_sem, per_sem)
    for i in range(lx):
        rows = pl.ds(i * ly, 2, stride=ly - 1)
        work[rows] = work[rows] + local[i]

    factor_z(0, lx // 3)

    for copy in mats_x:
        copy.wait()
    zeros = jnp.zeros_like(mat_x[0, 2])
    outer_x[0, 0] = zeros
    outer_x[1, 0] = zeros
    outer_x[2, 0] = zeros
    ratios = [zeros]
    joined = mat_x[0, 2]
    for q in range(1, half):
        link = 4.0 / (mat_x[q - 1, 4] + mat_x[q, 3])
        inverse = 1.0 / (link + joined + mat_x[q, 0])
        ratio = mat_x[q, 1] * inverse
        outer_x[0, q] = inverse
        outer_x[1, q] = ratio
        ratios.append(ratio)
        joined = mat_x[q, 2] - mat_x[q, 1] * ratio
    mid_out[0] = joined
    mid_out[1] = mat_x[half - 1, 4]
    mids = remote(mid_out, mid_in, mid_sem.at[0], mid_sem.at[1], mirror)

    for copy in mats_y:
        copy.wait()
    links = [4.0 / (mat_y[k, 4] + mat_y[k + 1, 3]) for k in range(ny - 1)]
    blank = jnp.zeros_like(links[0])
    alpha_y[0] = blank
    own_y[0, 0] = blank
    joined = mat_y[0, 2]
    for k in range(1, ny):
        inverse = 1.0 / (links[k - 1] + joined + mat_y[k, 0])
        ratio = mat_y[k, 1] * inverse
        alpha_y[k] = ratio
        own_y[0, k] = inverse
        joined = mat_y[k, 2] - mat_y[k, 1] * ratio
    beta_y[ny - 1] = blank
    own_y[1, ny - 1] = blank
    joined = mat_y[ny - 1, 0]
    for k in range(ny - 2, -1, -1):
        inverse = 1.0 / (links[k] + joined + mat_y[k, 2])
        ratio = mat_y[k, 1] * inverse
        beta_y[k] = ratio
        own_y[1, k] = inverse
        joined = mat_y[k, 0] - mat_y[k, 1] * ratio

    for copy in parts_x + parts_e:
        copy.wait()
    for q in range(half):
        for side in range(2):
            part_x[q, side, pair] = part_x[q, side, pair] + part_e[q, side]
    near, far = part_x[rank, 0], part_x[rank, 1]
    before = part_x[0, 1]
    for q in range(1, half):
        outer_x[2, q] = before
        before = part_x[q, 1] + ratios[q] * (before - part_x[q, 0])
    chain_out[...] = before
    chained = remote(chain_out, chain_in, mid_sem.at[2], mid_sem.at[3], mirror)
    factor_z(lx // 3, 2 * lx // 3)

    mids.wait()
    joined = mid_in[0]
    beyond = mid_in[1]
    ratios = [None] * half
    for q in range(half - 1, -1, -1):
        inverse = 1.0 / (4.0 / (mat_x[q, 4] + beyond) + joined + mat_x[q, 2])
        ratio = mat_x[q, 1] * inverse
        inner_x[0, q] = inverse
        inner_x[1, q] = ratio
        ratios[q] = ratio
        joined = mat_x[q, 0] - mat_x[q, 1] * ratio
        beyond = mat_x[q, 3]
    a, b = outer_x[1, rank], inner_x[1, rank]
    scale = 1.0 / (1.0 - a * b)
    gain_near = scale * outer_x[0, rank]
    gain_far = scale * inner_x[0, rank]
    left = outer_x[2, rank] - near
    chained.wait()
    after = chain_in[...]
    for q in range(half - 1, -1, -1):
        inner_x[2, q] = after
        if q:
            after = part_x[q, 0] + ratios[q] * (after - part_x[q, 1])
    right = far - inner_x[2, rank]
    into = gain_near * (left + b * right)
    out = gain_far * (right + a * left)
    on_head, on_tail = turn(into, -out)
    for i in range(lx):
        work[row_x(i)] += on_head * head_x[i] + on_tail * tail_x[i]

    local = substitute([work[row_y(j)] for j in range(ly)],
                       [None] + [mult_y[j] for j in range(1, ly)],
                       [inv_y[j] for j in range(ly)])
    head, tail = local[0], local[-1]
    a, b = alpha_y[iy], beta_y[iy]
    out_y[0] = tail - a * head
    out_y[1] = head - b * tail
    part_y[iy] = head
    copies = spread(lambda k: out_y.at[lax.div(iy + k, ny)], part_y, iy, peer_y, ny,
                    pys_sem, pyr_sem)
    for j in range(ly):
        work[row_y(j)] = local[j]
    factor_z(2 * lx // 3, lx)
    scale = 1.0 / (1.0 - a * b)
    gain_in, gain_out = scale * own_y[0, iy], scale * own_y[1, iy]
    for copy in copies:
        copy.wait()
    before = blank
    for k in range(ny - 1):
        before = jnp.where(k < iy, alpha_y[k] * before + part_y[k], before)
    after = blank
    for k in range(ny - 1, 0, -1):
        after = jnp.where(k > iy, beta_y[k] * after + part_y[k], after)
    left = before - head
    right = tail - after
    into = gain_in * (left + b * right)
    out = gain_out * (right + a * left)
    for j in range(ly):
        work[row_y(j)] += into * head_y[j] - out * tail_y[j]

    shift, level = 1, 0
    right = work[...]
    while shift < depth:
        right = (right + pcr_lo[level] * pltpu.roll(right, shift, 1)
                 + pcr_hi[level] * pltpu.roll(right, depth - shift, 1))
        shift, level = 2 * shift, level + 1
    o_ref[...] = f_ref[...] + right * pcr_inv[...]


def solution(mesh):
    nx, ny = mesh.shape["gx"], mesh.shape["gy"]

    def body(field, conductance, source):
        lx, ly, depth = field.shape
        lines = lx * ly
        levels = max(1, (depth - 1).bit_length())
        f32 = jnp.float32

        def vmem(*shape):
            return pltpu.VMEM(shape, f32)

        def dma(count):
            return pltpu.SemaphoreType.DMA((count,))

        half = nx // 2
        along_x = [vmem(lx, ly, depth)] * 4
        along_y = [vmem(ly, lx, depth)] * 4
        out = pl.pallas_call(
            functools.partial(kernel, nx, ny, lx, ly, depth),
            out_shape=pltpu.VMEM((lines, depth), f32),
            in_specs=[pl.BlockSpec(memory_space=pltpu.HBM)] * 3,
            out_specs=pl.BlockSpec(memory_space=pltpu.VMEM),
            scratch_shapes=[vmem(lines, depth)] * 3 + along_x + along_y + [
                vmem(levels, lines, depth), vmem(levels, lines, depth), vmem(lines, depth),
                vmem(lines, depth), vmem(2, 2, lx, depth), vmem(2, 2, lx, depth),
                vmem(half, 5, ly, depth), vmem(ny, 5, lx, depth),
                vmem(3, half, ly, depth), vmem(3, half, ly, depth),
                vmem(ny, lx, depth), vmem(ny, lx, depth), vmem(2, ny, lx, depth),
                vmem(half, 2, ly, depth), vmem(ny, lx, depth), vmem(2, lx, depth),
                vmem(2, ly, depth), vmem(2, ly, depth), vmem(ly, depth), vmem(ly, depth),
                vmem(2 * lx, depth), vmem(half, 2, 2, depth), dma(half - 1), dma(half - 1),
                dma(3), dma(2), dma(2), dma(half - 1), dma(half - 1), dma(ny - 1), dma(ny - 1),
                dma(half - 1), dma(half - 1), dma(ny - 1), dma(ny - 1), dma(4),
            ],
            compiler_params=pltpu.CompilerParams(
                collective_id=0, has_side_effects=True),
            name="step",
        )(field.reshape(lines, depth), conductance.reshape(lines, depth),
          source.reshape(lines, depth))
        return out.reshape(lx, ly, depth)

    spec = P("gx", "gy", None)
    return jax.shard_map(body, mesh=mesh, in_specs=(spec, spec, spec), out_specs=spec,
                         check_vma=False)
```
